32 devices in a mesh: span: 4 (over z), head: 4 (over y, x), group: 2 (over core).
Axes of the slice: x: 2, y: 2, z: 4, core: 2. Of those that a mesh axis runs over, the one named last changes fastest.
Arguments:
- states: bfloat16 [4096, 4096], P(('span', 'group'), 'head'), may hold values from -6 to 6
- owners: int32 [64, 2], P(('span', 'group')), may hold values from 0 to 3, as said below
- places: int32 [64, 2], P(('span', 'group')), may hold values from 0 to 7, as said below
- stored: bfloat16 [4, 4, 2, 8, 128, 896], P('span', 'head', 'group'), may hold values from -6 to 6
- encoder_weights: bfloat16 [896, 5376], P(('span', 'group')), may hold values from -0.1875 to 0.1875
- context_weight: bfloat16 [4096, 1792], P('head'), may hold values from -0.09375 to 0.09375
- query_weight: bfloat16 [4096, 4096], P(None, 'head'), may hold values from -0.09375 to 0.09375
- neighbour_weight: bfloat16 [896, 2, 4096], P(None, None, 'head'), may hold values from -0.1875 to 0.1875
- output_weight: bfloat16 [4096, 4096], P('head'), may hold values from -0.09375 to 0.09375
Outputs:
- updated: bfloat16 [4096, 4096], P(('span', 'group'), 'head')
The draws below stay inside these ranges and needn't reach their ends.
Inputs may be any that keep to these rules, and one draw needn't show every extreme that they name: `owners`: within each aligned block of 8 spans no two neighbours share an owner and a slot, no owner stores more than 8 of the block's neighbours, and at least one owner stores exactly 8. `places`: slots of a block's neighbours on one owner are distinct.
All inputs are finite; a program needn't handle non-finite values.
Results may differ from the reference program's by a relative error of at most 0.025.
Values may be sent and summed in bfloat16 or wider, within the bound.
No kernel may reach another device: no remote copies, remote signals or barrier semaphores. Data moves between devices by JAX's collectives and lax.ppermute only.
A program may use at most 128 MiB of HBM per device.

```python
import jax
import jax.numpy as jnp
from jax import lax

D = 4096
HEADS = 32
HEAD_DIM = 128
ENC_WIDTH = 896
SPAN_LEN = 64
RETRIEVED = 128
NEIGHBOURS = 2
BLOCK_SPANS = 8
QUERY_WIDTH = 4096
SPANS = 64
TOKENS = 4096
STORE_SLOTS = 8
N_SPAN = 4
N_HEAD = 4
N_GROUP = 2


def neighbour_places(key):
    block_count = SPANS // BLOCK_SPANS
    needed = BLOCK_SPANS * NEIGHBOURS
    holders = N_HEAD * STORE_SLOTS

    def one_block(block_key):
        first_key, second_key, third_key = jax.random.split(block_key, 3)
        busiest = jax.random.randint(first_key, (), 0, N_HEAD)
        shuffled = jax.random.permutation(second_key, holders)
        ranking = jnp.where(shuffled // STORE_SLOTS == busiest, 0, 1)
        ordered = shuffled[jnp.argsort(ranking, stable=True)]
        chosen = ordered[:needed]
        return chosen[jax.random.permutation(third_key, needed)]
    block_keys = jax.random.split(jax.random.fold_in(key, 11), block_count)
    return jax.vmap(one_block)(block_keys).reshape(SPANS, NEIGHBOURS).astype(jnp.int32)


def draw_owners(key, part):
    return neighbour_places(key) // STORE_SLOTS


def draw_places(key, part):
    return neighbour_places(key) % STORE_SLOTS


def steps_of(rng, dims, cuts, least, largest):
    def one(dim, blocks):
        steps = jax.random.uniform(jax.random.fold_in(jax.random.fold_in(rng, 6), dim), (blocks,), jnp.float32, least / len(cuts), largest / len(cuts))
        return jnp.repeat(jnp.exp(steps), dims[dim] // blocks).reshape((-1,) + (1,) * (len(dims) - dim - 1))

    factor_of = one(*cuts[0])
    for cut in cuts[1:]:
        factor_of = factor_of * one(*cut)
    return factor_of


def centred(stream_key, shape, deviation, limit, cuts=(), kind=jnp.bfloat16):
    array = deviation * jax.random.normal(stream_key, shape, jnp.float32)
    if cuts:
        array = array * steps_of(stream_key, shape, cuts, -0.22, 0.18)
    return jnp.clip(array, -limit, limit).astype(kind)


def setup_inputs(seed: int = 0) -> dict:
    splits = jax.random.split(jax.random.key(seed), 10)
    return {
        "states": centred(splits[0], (TOKENS, D), 1.0, 6.0, ((0, 8), (1, 4))),
        "owners": draw_owners(jax.random.fold_in(splits[9], 71), 0),
        "places": draw_places(jax.random.fold_in(splits[9], 71), 0),
        "stored": centred(splits[3], (N_SPAN, N_HEAD, N_GROUP, STORE_SLOTS, RETRIEVED, ENC_WIDTH), 1.0, 6.0, ((0, 4), (1, 4), (2, 2))),
        "encoder_weights": centred(splits[4], (ENC_WIDTH, 6 * ENC_WIDTH), ENC_WIDTH ** -0.5, 0.1875, ((0, 8),)),
        "context_weight": centred(splits[5], (D, 2 * ENC_WIDTH), D ** -0.5, 0.09375, ((0, 4),)),
        "query_weight": centred(splits[6], (D, QUERY_WIDTH), D ** -0.5, 0.09375, ((1, 4),)),
        "neighbour_weight": centred(splits[7], (ENC_WIDTH, 2, QUERY_WIDTH), ENC_WIDTH ** -0.5, 0.1875, ((2, 4),)),
        "output_weight": centred(splits[8], (QUERY_WIDTH, D), QUERY_WIDTH ** -0.5, 0.09375, ((0, 4),)),
    }


def attend(queries, keys_in, values_in, factor):
    scores = jnp.einsum("bqhe,bkhe->bhqk", queries.astype(jnp.float32), keys_in.astype(jnp.float32)) * factor
    weights = jax.nn.softmax(scores, axis=-1).astype(jnp.bfloat16)
    result = jnp.einsum("bhqk,bkhe->bqhe", weights.astype(jnp.float32), values_in.astype(jnp.float32))
    return result.astype(jnp.bfloat16)


def encode(source, context, weights):
    number, length, breadth = source.shape
    groups = breadth // HEAD_DIM
    factor = HEAD_DIM ** -0.5
    rows_in = source.reshape(number * length, breadth)
    triple = jnp.dot(rows_in, weights[:, :3 * breadth], preferred_element_type=jnp.float32).astype(jnp.bfloat16)
    triple = triple.reshape(number, length, 3, groups, HEAD_DIM)
    within = attend(triple[:, :, 0], triple[:, :, 1], triple[:, :, 2], factor).reshape(number * length, breadth)
    middle = rows_in.astype(jnp.float32) + jnp.dot(within, weights[:, 3 * breadth:4 * breadth], preferred_element_type=jnp.float32)
    middle = middle.astype(jnp.bfloat16)
    asking = jnp.dot(middle, weights[:, 4 * breadth:5 * breadth], preferred_element_type=jnp.float32).astype(jnp.bfloat16)
    asking = asking.reshape(number, length, groups, HEAD_DIM)
    paired = context.reshape(number, context.shape[1], 2, groups, HEAD_DIM)
    across = attend(asking, paired[:, :, 0], paired[:, :, 1], factor).reshape(number * length, breadth)
    result = middle.astype(jnp.float32) + jnp.dot(across, weights[:, 5 * breadth:], preferred_element_type=jnp.float32)
    return result.astype(jnp.bfloat16).reshape(number, length, breadth)


def reference(states, owners, places, stored, encoder_weights, context_weight, query_weight, neighbour_weight, output_weight):
    factor = HEAD_DIM ** -0.5
    context = jnp.dot(states, context_weight, preferred_element_type=jnp.float32).astype(jnp.bfloat16)
    context = context.reshape(SPANS, SPAN_LEN, 2 * ENC_WIDTH)
    blocks = jnp.arange(SPANS, dtype=jnp.int32) // BLOCK_SPANS
    span_index = (blocks // N_GROUP)[:, None]
    group_index = (blocks % N_GROUP)[:, None]
    source = stored[span_index, owners, group_index, places].reshape(SPANS * NEIGHBOURS, RETRIEVED, ENC_WIDTH)
    repeated = jnp.repeat(context, NEIGHBOURS, axis=0)
    encoded = encode(source, repeated, encoder_weights)
    neighbour_pairs = jnp.dot(encoded.reshape(SPANS * NEIGHBOURS * RETRIEVED, ENC_WIDTH), neighbour_weight.reshape(ENC_WIDTH, 2 * QUERY_WIDTH), preferred_element_type=jnp.float32).astype(jnp.bfloat16)
    memory = neighbour_pairs.reshape(SPANS, NEIGHBOURS * RETRIEVED, 2, HEADS, HEAD_DIM)
    queries = jnp.dot(states, query_weight, preferred_element_type=jnp.float32).astype(jnp.bfloat16)
    queries = queries.reshape(SPANS, SPAN_LEN, HEADS, HEAD_DIM)
    attended = attend(queries, memory[:, :, 0], memory[:, :, 1], factor).reshape(TOKENS, QUERY_WIDTH)
    group_width = QUERY_WIDTH // N_HEAD

    def add_group(group_number, running):
        start = (group_number * group_width).astype(jnp.int32)
        columns = lax.dynamic_slice_in_dim(attended, start, group_width, 1)
        rows_of = lax.dynamic_slice_in_dim(output_weight, start, group_width, 0)
        partial_term = jnp.dot(columns, rows_of, preferred_element_type=jnp.float32).astype(jnp.bfloat16)
        partial_term = lax.optimization_barrier(partial_term)
        return running + partial_term.astype(jnp.float32)

    summed = lax.fori_loop(0, N_HEAD, add_group, jnp.zeros((TOKENS, D), jnp.float32))
    return (states.astype(jnp.float32) + summed).astype(jnp.bfloat16)
```

```python
import functools

import jax
import jax.numpy as jnp
from jax import lax
from jax.experimental import pallas as pl
from jax.experimental.pallas import tpu as pltpu
from jax.sharding import PartitionSpec as P

HEAD_DIM = 128
ENC_WIDTH = 896
SPAN_LEN = 64
RETRIEVED = 128
NEIGHBOURS = 2

VMEM_LIMIT = 60 * 1024 * 1024

ANY = pl.BlockSpec(memory_space=pl.ANY)
VMEM = pl.BlockSpec(memory_space=pltpu.VMEM)
SMEM = pl.BlockSpec(memory_space=pltpu.SMEM)


def attend(queries, keys_in, values_in, factor):
    scores = (
        jnp.einsum("bqhe,bkhe->bhqk", queries, keys_in, preferred_element_type=jnp.float32) * factor
    )
    weights = jax.nn.softmax(scores, axis=-1).astype(jnp.bfloat16)
    result = jnp.einsum("bhqk,bkhe->bqhe", weights, values_in, preferred_element_type=jnp.float32)
    return result.astype(jnp.bfloat16)


def encode(source, context, weights):
    number, length, breadth = source.shape
    groups = breadth // HEAD_DIM
    factor = HEAD_DIM ** (-0.5)
    rows_in = source.reshape(number * length, breadth)
    triple = jnp.dot(rows_in, weights[:, : 3 * breadth], preferred_element_type=jnp.float32).astype(
        jnp.bfloat16
    )
    triple = triple.reshape(number, length, 3, groups, HEAD_DIM)
    within = attend(triple[:, :, 0], triple[:, :, 1], triple[:, :, 2], factor).reshape(
        number * length, breadth
    )
    middle = rows_in.astype(jnp.float32) + jnp.dot(
        within, weights[:, 3 * breadth : 4 * breadth], preferred_element_type=jnp.float32
    )
    middle = middle.astype(jnp.bfloat16)
    asking = jnp.dot(
        middle, weights[:, 4 * breadth : 5 * breadth], preferred_element_type=jnp.float32
    ).astype(jnp.bfloat16)
    asking = asking.reshape(number, length, groups, HEAD_DIM)
    paired = context.reshape(number, context.shape[1], 2, groups, HEAD_DIM)
    across = attend(asking, paired[:, :, 0], paired[:, :, 1], factor).reshape(
        number * length, breadth
    )
    result = middle.astype(jnp.float32) + jnp.dot(
        across, weights[:, 5 * breadth :], preferred_element_type=jnp.float32
    )
    return result.astype(jnp.bfloat16).reshape(number, length, breadth)


def general(
    states,
    owners,
    places,
    stored,
    encoder_weights,
    context_weight,
    query_weight,
    neighbour_weight,
    output_weight,
):
    position = lax.axis_index("head")
    token_rows = states.shape[0]
    span_count = owners.shape[0]
    pair_count = span_count * NEIGHBOURS
    local_width = query_weight.shape[1]
    local_heads = local_width // HEAD_DIM
    factor = HEAD_DIM ** (-0.5)
    query_sums = jnp.dot(
        lax.all_gather(states, "head", axis=1, tiled=True),
        query_weight,
        preferred_element_type=jnp.float32,
    )
    queries = query_sums.astype(jnp.bfloat16)
    partial_context = jnp.dot(states, context_weight, preferred_element_type=jnp.float32)
    context = lax.psum(partial_context.astype(jnp.bfloat16), "head")
    context = context.reshape(span_count, SPAN_LEN, 2 * ENC_WIDTH)
    weights_all = lax.all_gather(encoder_weights, ("span", "group"), axis=0, tiled=True)
    owner_flat = owners.reshape(pair_count)
    place_flat = places.reshape(pair_count)
    pair_ids = jnp.arange(pair_count, dtype=jnp.int32)
    local_store = stored.reshape(stored.shape[3], stored.shape[4], stored.shape[5])
    slot_count = local_store.shape[0]
    slot_ids = jnp.arange(slot_count, dtype=jnp.int32)
    matched = (owner_flat[None, :] == position) & (place_flat[None, :] == slot_ids[:, None])
    span_of = jnp.sum(jnp.where(matched, pair_ids[None, :] // NEIGHBOURS, 0), axis=1)
    encoded = encode(local_store, context[span_of], weights_all)
    local_pair = neighbour_weight.reshape(ENC_WIDTH, 2 * local_width)
    piece = lax.all_gather(encoded, "head", axis=0, tiled=True)
    rows_in = piece.reshape(piece.shape[0] * RETRIEVED, ENC_WIDTH)
    result = jnp.dot(rows_in, local_pair, preferred_element_type=jnp.float32).astype(jnp.bfloat16)
    gathered = result.reshape(piece.shape[0], RETRIEVED, 2 * local_width)
    neighbour_pairs = gathered[owner_flat * slot_count + place_flat]
    asked = queries.reshape(span_count, SPAN_LEN, local_heads, HEAD_DIM)
    memory = neighbour_pairs.reshape(span_count, NEIGHBOURS * RETRIEVED, 2, local_heads, HEAD_DIM)
    attended = attend(asked, memory[:, :, 0], memory[:, :, 1], factor).reshape(
        token_rows, local_width
    )
    terms = jnp.dot(attended, output_weight, preferred_element_type=jnp.float32)
    summed = lax.psum_scatter(
        terms.astype(jnp.bfloat16), "head", scatter_dimension=1, tiled=True
    ).astype(jnp.float32)
    return (states.astype(jnp.float32) + summed).astype(jnp.bfloat16)


def call(kernel, out_shape, in_specs, out_specs, scratch, flops, moved, *args):
    return pl.pallas_call(
        kernel,
        out_shape=out_shape,
        in_specs=in_specs,
        out_specs=out_specs,
        scratch_shapes=scratch,
        compiler_params=pltpu.CompilerParams(vmem_limit_bytes=VMEM_LIMIT),
        cost_estimate=pl.CostEstimate(flops=flops, bytes_accessed=moved, transcendentals=0),
    )(*args)


def dot(a, b):
    return jnp.dot(a, b, preferred_element_type=jnp.float32)


def one_head(q, k, v):
    scores = lax.dot_general(
        q, k, (((1,), (1,)), ((), ())), preferred_element_type=jnp.float32
    ) * (HEAD_DIM ** (-0.5))
    top = jnp.max(scores, axis=-1, keepdims=True)
    e = jnp.exp(scores - top)
    w = (e / jnp.sum(e, axis=-1, keepdims=True)).astype(jnp.bfloat16)
    return dot(w, v).astype(jnp.bfloat16)


def pick_kernel(idx, store, *rest):
    outs, (buf, sem_in, sem_out) = rest[:3], rest[3:]
    per = outs[0].shape[0]
    ins = [
        pltpu.make_async_copy(store.at[idx[i]], buf.at[i], sem_in.at[i]) for i in range(3 * per)
    ]
    for c in ins:
        c.start()
    puts = [
        pltpu.make_async_copy(buf.at[i], outs[i // per].at[i % per], sem_out.at[i])
        for i in range(3 * per)
    ]
    for i in range(3 * per):
        ins[i].wait()
        puts[i].start()
    for c in puts:
        c.wait()


def context_kernel(meta, x, w, *rest):
    outs, buf = rest[:4], rest[4]
    width = w.shape[1]
    rows = outs[0].shape[0]
    half = width // 2
    for c in range(2):
        cols = slice(c * half, (c + 1) * half)
        buf[:, cols] = dot(x[...], w[:, cols]).astype(jnp.bfloat16)
    for k in range(4):
        start = pl.multiple_of((meta[0] ^ k) * rows, rows)
        outs[k][...] = buf[pl.ds(start, rows), :]


def load_pieces(meta, first, pieces, held, sems):
    rows = pieces[0].shape[0]
    copies = []
    for i, piece in enumerate(pieces):
        start = pl.multiple_of(meta[first + i] * rows, rows)
        copies.append(
            pltpu.make_async_copy(piece, held.at[pl.ds(start, rows), :], sems.at[i])
        )
    return copies


def self_kernel(n_pieces, meta, store, r1, r2, r3, *rest):
    pieces = rest[:n_pieces]
    source, within, held, triple, sem_s, sem_w = rest[n_pieces:]
    per = r1.shape[0]
    copies = load_pieces(meta, 2 * per, pieces, held, sem_w)
    for j in range(per):
        at = source.at[pl.ds(j * RETRIEVED, RETRIEVED), :]
        for k, ref in enumerate((store, r1, r2, r3)):

            @pl.when(meta[j] == k)
            def _():
                pltpu.make_async_copy(
                    ref.at[meta[per + j] if k == 0 else j], at, sem_s.at[j]
                ).start()

    for c in copies:
        c.start()
    for j in range(per):
        at = source.at[pl.ds(j * RETRIEVED, RETRIEVED), :]
        pltpu.make_async_copy(r1.at[j], at, sem_s.at[j]).wait()
    for c in copies:
        c.wait()
    breadth = source.shape[1]
    for c in range(3):
        cols = slice(c * breadth, (c + 1) * breadth)
        triple[:, cols] = dot(source[...], held[:, cols]).astype(jnp.bfloat16)
    for j in range(per):
        rows = slice(j * RETRIEVED, (j + 1) * RETRIEVED)
        for h in range(breadth // HEAD_DIM):
            c0 = h * HEAD_DIM
            within[rows, c0 : c0 + HEAD_DIM] = one_head(
                triple[rows, c0 : c0 + HEAD_DIM],
                triple[rows, breadth + c0 : breadth + c0 + HEAD_DIM],
                triple[rows, 2 * breadth + c0 : 2 * breadth + c0 + HEAD_DIM],
            )


def cross_kernel(n_pieces, meta, source, within, c0, c1, c2, c3, *rest):
    pieces = rest[:n_pieces]
    outs = rest[n_pieces:-6]
    held, context, middle, asking, across, sem_w = rest[-6:]
    copies = load_pieces(meta, 0, pieces, held, sem_w)
    for c in copies:
        c.start()
    breadth = source.shape[1]
    total = c0[...].astype(jnp.float32) + c1[...].astype(jnp.float32)
    total = total + (c2[...].astype(jnp.float32) + c3[...].astype(jnp.float32))
    context[...] = total.astype(jnp.bfloat16)
    for c in copies:
        c.wait()
    middle[...] = (
        source[...].astype(jnp.float32) + dot(within[...], held[:, :breadth])
    ).astype(jnp.bfloat16)
    asking[...] = dot(middle[...], held[:, breadth : 2 * breadth]).astype(jnp.bfloat16)
    span_rows = NEIGHBOURS * RETRIEVED
    for s in range(len(outs)):
        rows = slice(s * span_rows, (s + 1) * span_rows)
        keys = slice(s * SPAN_LEN, (s + 1) * SPAN_LEN)
        for h in range(breadth // HEAD_DIM):
            at = h * HEAD_DIM
            across[rows, at : at + HEAD_DIM] = one_head(
                asking[rows, at : at + HEAD_DIM],
                context[keys, at : at + HEAD_DIM],
                context[keys, breadth + at : breadth + at + HEAD_DIM],
            )
    for s, out in enumerate(outs):
        rows = slice(s * span_rows, (s + 1) * span_rows)
        out[...] = (
            middle[rows, :].astype(jnp.float32) + dot(across[rows, :], held[:, 2 * breadth :])
        ).astype(jnp.bfloat16)


def query_kernel(meta, own, x0, x1, y0, y1, d0, d1, w, out, held, total, sems):
    width = own.shape[1]
    half = x0.shape[0]
    copies = []
    for k in range(4):
        start = pl.multiple_of((meta[0] ^ k) * width, width)
        copies.append(
            pltpu.make_async_copy(w.at[pl.ds(start, width), :], held.at[k], sems.at[k])
        )
    for c in copies:
        c.start()
    copies[0].wait()
    total[...] = dot(own[...], held[0])
    for k, (a, b) in enumerate(((x0, x1), (y0, y1), (d0, d1))):
        copies[k + 1].wait()
        total[:half, :] += dot(a[...], held[k + 1])
        total[half:, :] += dot(b[...], held[k + 1])
    out[...] = total[...].astype(jnp.bfloat16)


def span_kernel(rel, meta, queries, *rest):
    n = len(rest) - 13
    encs = rest[:n]
    w_pair, w_out = rest[n : n + 2]
    outs = rest[n + 2 : n + 6]
    q, keep, pair, held, memory, att, sem = rest[n + 6 :]
    rows = n * SPAN_LEN
    local = q.shape[1]
    at = pl.multiple_of((meta[0] ^ rel) * rows, rows)
    load_q = pltpu.make_async_copy(queries.at[pl.ds(at, rows), :], q, sem.at[0])
    load_pair = pltpu.make_async_copy(w_pair, pair, sem.at[1])
    load_out = pltpu.make_async_copy(w_out, held, sem.at[2])
    load_pair.start()
    load_q.start()
    load_out.start()
    span_rows = NEIGHBOURS * RETRIEVED
    for s in range(n):
        keep[s * span_rows : (s + 1) * span_rows, :] = encs[s][...]
    load_pair.wait()
    for c in range(2):
        cols = slice(c * local, (c + 1) * local)
        memory[:, cols] = dot(keep[...], pair[:, cols]).astype(jnp.bfloat16)
    load_q.wait()
    for s in range(n):
        r = slice(s * SPAN_LEN, (s + 1) * SPAN_LEN)
        m = slice(s * span_rows, (s + 1) * span_rows)
        for h in range(local // HEAD_DIM):
            c0 = h * HEAD_DIM
            att[r, c0 : c0 + HEAD_DIM] = one_head(
                q[r, c0 : c0 + HEAD_DIM],
                memory[m, c0 : c0 + HEAD_DIM],
                memory[m, local + c0 : local + c0 + HEAD_DIM],
            )
    load_out.wait()
    width = outs[0].shape[1]
    for k in range(4):
        start = pl.multiple_of((meta[0] ^ k) * width, width)
        outs[k][...] = dot(att[...], held[:, pl.ds(start, width)]).astype(jnp.bfloat16)


def final_kernel(meta, states, *rest):
    terms, out = rest[:16], rest[16]
    rows = terms[0].shape[0]
    for m in range(4):
        at = pl.ds(pl.multiple_of((meta[0] ^ m) * rows, rows), rows)
        parts = [terms[4 * k + (k ^ m)][...].astype(jnp.float32) for k in range(4)]
        total = (parts[0] + parts[1]) + (parts[2] + parts[3])
        out[at, :] = (states[at, :].astype(jnp.float32) + total).astype(jnp.bfloat16)


def shape(*dims):
    return jax.ShapeDtypeStruct(dims, jnp.bfloat16)


def to(k, value):
    return lax.ppermute(value, "head", [(i, i ^ k) for i in range(4)])


def fast(
    n_span,
    states,
    owners,
    places,
    stored,
    encoder_weights,
    context_weight,
    query_weight,
    neighbour_weight,
    output_weight,
):
    bf16 = jnp.bfloat16
    h = lax.axis_index("head").astype(jnp.int32)
    z = lax.axis_index("span").astype(jnp.int32)
    g = lax.axis_index("group").astype(jnp.int32)
    tokens, feat = states.shape
    span_count = owners.shape[0]
    pairs = span_count * NEIGHBOURS
    per = pairs // 4
    own_spans = span_count // 4
    local = query_weight.shape[1]
    slots = stored.shape[3]
    store = stored.reshape(slots, RETRIEVED, ENC_WIDTH)
    owner_of = owners.reshape(4, per).astype(jnp.int32)
    place_of = places.reshape(4, per).astype(jnp.int32)
    me = h.reshape(1)

    rel = jnp.arange(1, 4, dtype=jnp.int32)
    idx = place_of[h ^ rel].reshape(3 * per)
    sends = call(
        pick_kernel,
        [shape(per, RETRIEVED, ENC_WIDTH)] * 3,
        [SMEM, ANY],
        [ANY] * 3,
        [
            pltpu.VMEM((3 * per, RETRIEVED, ENC_WIDTH), bf16),
            pltpu.SemaphoreType.DMA((3 * per,)),
            pltpu.SemaphoreType.DMA((3 * per,)),
        ],
        0,
        12 * per * RETRIEVED * ENC_WIDTH,
        idx,
        store,
    )
    raw = [to(k + 1, sends[k]) for k in range(3)]

    cut = 3 * ENC_WIDTH
    rows_w = encoder_weights.shape[0]
    ring = [(i, (i + 1) % n_span) for i in range(n_span)]
    halves = []
    for part in (encoder_weights[:, :cut], encoder_weights[:, cut:]):
        pieces, now = [], part
        for r in range(n_span):
            if r:
                now = lax.ppermute(now, "span", ring)
            pieces.append(now)
            pieces.append(lax.ppermute(now, "group", [(0, 1), (1, 0)]))
        halves.append(pieces)
    n_pieces = 2 * n_span
    spots = []
    for r in range(n_span):
        source_z = (z - r + n_span) % n_span
        spots += [source_z * 2 + g, source_z * 2 + (1 - g)]
    spots = jnp.stack(spots).astype(jnp.int32)

    width_c = context_weight.shape[1]
    rows_c = tokens // 4
    part_c = call(
        context_kernel,
        [shape(rows_c, width_c)] * 4,
        [SMEM, VMEM, VMEM],
        [VMEM] * 4,
        [pltpu.VMEM((tokens, width_c), bf16)],
        2 * tokens * feat * width_c,
        2 * (feat * width_c + tokens * feat + tokens * width_c),
        me,
        states,
        context_weight,
    )
    context = [part_c[0]] + [to(k, part_c[k]) for k in range(1, 4)]

    half_t = tokens // 2
    s0, s1 = states[:half_t], states[half_t:]
    x0, y1 = to(1, s0), to(2, s1)
    x1, y0 = to(1, s1), to(2, s0)
    d0, d1 = to(2, x0), to(1, y1)

    mine = place_of[h], owner_of[h] ^ h
    meta_a = jnp.concatenate([mine[1], mine[0], spots])
    source, within = call(
        functools.partial(self_kernel, n_pieces),
        [shape(per * RETRIEVED, ENC_WIDTH)] * 2,
        [SMEM] + [ANY] * (4 + n_pieces),
        [VMEM] * 2,
        [
            pltpu.VMEM((ENC_WIDTH, cut), bf16),
            pltpu.VMEM((per * RETRIEVED, cut), bf16),
            pltpu.SemaphoreType.DMA((per,)),
            pltpu.SemaphoreType.DMA((n_pieces,)),
        ],
        2 * per * RETRIEVED * ENC_WIDTH * cut * 2,
        2 * ENC_WIDTH * cut,
        meta_a,
        store,
        *raw,
        *halves[0],
    )
    span_rows = NEIGHBOURS * RETRIEVED
    enc = call(
        functools.partial(cross_kernel, n_pieces),
        [shape(span_rows, ENC_WIDTH)] * own_spans,
        [SMEM] + [VMEM] * 6 + [ANY] * n_pieces,
        [VMEM] * own_spans,
        [
            pltpu.VMEM((ENC_WIDTH, cut), bf16),
            pltpu.VMEM((rows_c, width_c), bf16),
            pltpu.VMEM((per * RETRIEVED, ENC_WIDTH), bf16),
            pltpu.VMEM((per * RETRIEVED, ENC_WIDTH), bf16),
            pltpu.VMEM((per * RETRIEVED, ENC_WIDTH), bf16),
            pltpu.SemaphoreType.DMA((n_pieces,)),
        ],
        2 * per * RETRIEVED * ENC_WIDTH * cut * 2,
        2 * ENC_WIDTH * cut,
        spots,
        source,
        within,
        *context,
        *halves[1],
    )
    first = own_spans // 2
    x = [to(1, e) for e in enc]
    y = [to(2, e) for e in enc]
    d = [to(2, e) for e in x[:first]] + [to(1, e) for e in y[first:]]

    queries = call(
        query_kernel,
        shape(tokens, local),
        [SMEM] + [VMEM] * 7 + [ANY],
        VMEM,
        [
            pltpu.VMEM((4, feat, local), bf16),
            pltpu.VMEM((tokens, local), jnp.float32),
            pltpu.SemaphoreType.DMA((4,)),
        ],
        2 * tokens * 4 * feat * local,
        2 * 4 * feat * local,
        me,
        states,
        x0,
        x1,
        y0,
        y1,
        d0,
        d1,
        query_weight,
    )
    w_pair = neighbour_weight.reshape(ENC_WIDTH, 2 * local)
    rows_q = own_spans * SPAN_LEN
    terms = []
    for rel_index, chunk in enumerate((enc, x, y, d)):
        terms.append(
            call(
                functools.partial(span_kernel, rel_index),
                [shape(rows_q, feat)] * 4,
                [SMEM, ANY] + [VMEM] * own_spans + [ANY] * 2,
                [VMEM] * 4,
                [
                    pltpu.VMEM((rows_q, local), bf16),
                    pltpu.VMEM((own_spans * span_rows, ENC_WIDTH), bf16),
                    pltpu.VMEM((ENC_WIDTH, 2 * local), bf16),
                    pltpu.VMEM(output_weight.shape, bf16),
                    pltpu.VMEM((own_spans * span_rows, 2 * local), bf16),
                    pltpu.VMEM((rows_q, local), bf16),
                    pltpu.SemaphoreType.DMA((3,)),
                ],
                4 * own_spans * span_rows * ENC_WIDTH * 2 * local,
                2 * (ENC_WIDTH * 2 * local + 4 * local * feat),
                me,
                queries,
                *chunk,
                w_pair,
                output_weight,
            )
        )
    arrived = []
    for k in range(4):
        for r in range(4):
            arrived.append(terms[r][k] if k == 0 else to(k, terms[r][k]))
    return call(
        final_kernel,
        shape(tokens, feat),
        [SMEM] + [VMEM] * 17,
        VMEM,
        [],
        17 * tokens * feat,
        10 * tokens * feat,
        me,
        states,
        *arrived,
    )


def solution(mesh):
    sizes = mesh.shape
    n_head = sizes["head"]

    def per_device(*args):
        spans = args[1].shape[0]
        if n_head == 4 and sizes["group"] == 2 and spans % 8 == 0:
            return fast(sizes["span"], *args)
        return general(*args)

    in_specs = (
        P(("span", "group"), "head"),
        P(("span", "group"), None),
        P(("span", "group"), None),
        P("span", "head", "group", None, None, None),
        P(("span", "group"), None),
        P("head", None),
        P(None, "head"),
        P(None, None, "head"),
        P("head", None),
    )
    out_specs = P(("span", "group"), "head")
    return jax.shard_map(
        per_device, mesh=mesh, in_specs=in_specs, out_specs=out_specs, check_vma=False
    )
```

```python
import functools

import jax
import jax.numpy as jnp
import numpy as np
from jax import lax
from jax.experimental import pallas as pl
from jax.experimental.pallas import tpu as pltpu
from jax.sharding import PartitionSpec as P


HEAD_DIM = 128
ENC_WIDTH = 896
SPAN_LEN = 64
RETRIEVED = 128
NEIGHBOURS = 2


HBM = pl.BlockSpec(memory_space=pltpu.HBM)
VMEM = pl.BlockSpec(memory_space=pltpu.VMEM)
SMEM = pl.BlockSpec(memory_space=pltpu.SMEM)


def attend(queries, keys_in, values_in, factor):
    scores = (
        jnp.einsum("bqhe,bkhe->bhqk", queries, keys_in, preferred_element_type=jnp.float32) * factor
    )
    weights = jax.nn.softmax(scores, axis=-1).astype(jnp.bfloat16)
    result = jnp.einsum("bhqk,bkhe->bqhe", weights, values_in, preferred_element_type=jnp.float32)
    return result.astype(jnp.bfloat16)


def encode(source, context, weights):
    number, length, breadth = source.shape
    groups = breadth // HEAD_DIM
    factor = HEAD_DIM ** (-0.5)
    rows_in = source.reshape(number * length, breadth)
    triple = jnp.dot(rows_in, weights[:, : 3 * breadth], preferred_element_type=jnp.float32).astype(
        jnp.bfloat16
    )
    triple = triple.reshape(number, length, 3, groups, HEAD_DIM)
    within = attend(triple[:, :, 0], triple[:, :, 1], triple[:, :, 2], factor).reshape(
        number * length, breadth
    )
    middle = rows_in.astype(jnp.float32) + jnp.dot(
        within, weights[:, 3 * breadth : 4 * breadth], preferred_element_type=jnp.float32
    )
    middle = middle.astype(jnp.bfloat16)
    asking = jnp.dot(
        middle, weights[:, 4 * breadth : 5 * breadth], preferred_element_type=jnp.float32
    ).astype(jnp.bfloat16)
    asking = asking.reshape(number, length, groups, HEAD_DIM)
    paired = context.reshape(number, context.shape[1], 2, groups, HEAD_DIM)
    across = attend(asking, paired[:, :, 0], paired[:, :, 1], factor).reshape(
        number * length, breadth
    )
    result = middle.astype(jnp.float32) + jnp.dot(
        across, weights[:, 5 * breadth :], preferred_element_type=jnp.float32
    )
    return result.astype(jnp.bfloat16).reshape(number, length, breadth)


def general(
    states,
    owners,
    places,
    stored,
    encoder_weights,
    context_weight,
    query_weight,
    neighbour_weight,
    output_weight,
):
    position = lax.axis_index("head")
    token_rows = states.shape[0]
    span_count = owners.shape[0]
    pair_count = span_count * NEIGHBOURS
    local_width = query_weight.shape[1]
    local_heads = local_width // HEAD_DIM
    factor = HEAD_DIM ** (-0.5)
    query_sums = jnp.dot(
        lax.all_gather(states, "head", axis=1, tiled=True),
        query_weight,
        preferred_element_type=jnp.float32,
    )
    queries = query_sums.astype(jnp.bfloat16)
    partial_context = jnp.dot(states, context_weight, preferred_element_type=jnp.float32)
    context = lax.psum(partial_context.astype(jnp.bfloat16), "head")
    context = context.reshape(span_count, SPAN_LEN, 2 * ENC_WIDTH)
    weights_all = lax.all_gather(encoder_weights, ("span", "group"), axis=0, tiled=True)
    owner_flat = owners.reshape(pair_count)
    place_flat = places.reshape(pair_count)
    pair_ids = jnp.arange(pair_count, dtype=jnp.int32)
    local_store = stored.reshape(stored.shape[3], stored.shape[4], stored.shape[5])
    slot_count = local_store.shape[0]
    slot_ids = jnp.arange(slot_count, dtype=jnp.int32)
    matched = (owner_flat[None, :] == position) & (place_flat[None, :] == slot_ids[:, None])
    span_of = jnp.sum(jnp.where(matched, pair_ids[None, :] // NEIGHBOURS, 0), axis=1)
    encoded = encode(local_store, context[span_of], weights_all)
    local_pair = neighbour_weight.reshape(ENC_WIDTH, 2 * local_width)
    piece = lax.all_gather(encoded, "head", axis=0, tiled=True)
    rows_in = piece.reshape(piece.shape[0] * RETRIEVED, ENC_WIDTH)
    result = jnp.dot(rows_in, local_pair, preferred_element_type=jnp.float32).astype(jnp.bfloat16)
    gathered = result.reshape(piece.shape[0], RETRIEVED, 2 * local_width)
    neighbour_pairs = gathered[owner_flat * slot_count + place_flat]
    asked = queries.reshape(span_count, SPAN_LEN, local_heads, HEAD_DIM)
    memory = neighbour_pairs.reshape(span_count, NEIGHBOURS * RETRIEVED, 2, local_heads, HEAD_DIM)
    attended = attend(asked, memory[:, :, 0], memory[:, :, 1], factor).reshape(
        token_rows, local_width
    )
    terms = jnp.dot(attended, output_weight, preferred_element_type=jnp.float32)
    summed = lax.psum_scatter(
        terms.astype(jnp.bfloat16), "head", scatter_dimension=1, tiled=True
    ).astype(jnp.float32)
    return (states.astype(jnp.float32) + summed).astype(jnp.bfloat16)


def call(kernel, out_shape, in_specs, out_specs, scratch, mib, flops, *args):
    return pl.pallas_call(
        kernel,
        out_shape=out_shape,
        in_specs=in_specs,
        out_specs=out_specs,
        scratch_shapes=scratch,
        compiler_params=pltpu.CompilerParams(vmem_limit_bytes=mib * 1024 * 1024),
        cost_estimate=pl.CostEstimate(
            flops=flops,
            bytes_accessed=2 * sum(a.size for a in args),
            transcendentals=0,
        ),
    )(*args)


def dot(a, b):
    return jnp.dot(a, b, preferred_element_type=jnp.float32)


def attend_many(units, scores, weights):
    rows = scores.shape[0] // len(units)
    part = [slice(i * rows, (i + 1) * rows) for i in range(len(units))]
    factor = HEAD_DIM ** (-0.5)
    for at, (q, k, _, _) in zip(part, units):
        scores[at, :] = lax.dot_general(
            q(), k(), (((1,), (1,)), ((), ())), preferred_element_type=jnp.float32
        )
    for at in part:
        one = scores[at, :]
        top = jnp.max(one, axis=-1, keepdims=True)
        weights[at, :] = jnp.exp((one - top) * factor).astype(jnp.bfloat16)
    for at, (_, _, v, put) in zip(part, units):
        values = v()
        both = dot(weights[at, :], jnp.concatenate([values, jnp.ones_like(values)], axis=1))
        put((both[:, :HEAD_DIM] / both[:, HEAD_DIM:]).astype(jnp.bfloat16))


def unit(q, q_rows, q_col, k, k_rows, k_col, v_col, out):
    def put(value):
        out[q_rows, q_col : q_col + HEAD_DIM] = value

    return (
        lambda: q[q_rows, q_col : q_col + HEAD_DIM],
        lambda: k[k_rows, k_col : k_col + HEAD_DIM],
        lambda: k[k_rows, v_col : v_col + HEAD_DIM],
        put,
    )


def head_index():
    return lax.axis_index("head").astype(jnp.int32)


def pairings(items):
    if not items:
        yield ()
        return
    for other in items[1:]:
        rest = tuple(i for i in items[1:] if i != other)
        for more in pairings(rest):
            yield ((items[0], other),) + more


def pair_table(spans):
    every = list(pairings(tuple(range(spans))))
    table = np.full((spans, -(-len(every) // 128) * 128), -1, np.int32)
    for c, pairing in enumerate(every):
        for slot, pair in enumerate(pairing):
            for span in pair:
                table[span, c] = slot
    return table


def plan_kernel(owners, table, assign):
    spans = table.shape[0]
    devices = spans // 2
    shape_row = (1, table.shape[1])
    hits = [
        [sum((owners[n, s] == o).astype(jnp.int32) for n in range(NEIGHBOURS)) for s in range(spans)]
        for o in range(devices)
    ]
    rows = [table[s : s + 1, :] for s in range(spans)]
    inside = [[(r == slot).astype(jnp.int32) for r in rows] for slot in range(devices)]
    fits = rows[0] >= 0
    for o in range(devices):
        heavy = jnp.zeros(shape_row, jnp.int32)
        for slot in range(devices):
            count = jnp.zeros(shape_row, jnp.int32)
            for s in range(spans):
                count = count + inside[slot][s] * hits[o][s]
            heavy = heavy + (count >= 3).astype(jnp.int32)
        fits = fits & (heavy <= 1)
    code = jnp.zeros(shape_row, jnp.int32)
    for s in range(spans):
        code = code + rows[s] * (devices**s)
    worst = devices**spans
    chosen = jnp.min(jnp.where(fits, code, worst).astype(jnp.float32)).astype(jnp.int32)
    slot_of = []
    for s in range(spans):
        slot_of.append(lax.rem(chosen, devices))
        chosen = lax.div(chosen, devices)
    takes = []
    for slot in range(devices):
        taker = jnp.int32(-1)
        for o in range(devices):
            count = sum(jnp.where(slot_of[s] == slot, hits[o][s], 0) for s in range(spans))
            taker = jnp.where(count >= 3, o, taker)
        takes.append(taker)
    for slot in range(devices):
        free = jnp.int32(0)
        for d in reversed(range(devices)):
            taken = sum((t == d).astype(jnp.int32) for t in takes)
            free = jnp.where(taken == 0, d, free)
        takes[slot] = jnp.where(takes[slot] < 0, free, takes[slot])
    for s in range(spans):
        before = sum(((slot_of[t] == slot_of[s]).astype(jnp.int32) for t in range(s)), jnp.int32(0))
        device = jnp.int32(0)
        for slot in range(devices):
            device = jnp.where(slot_of[s] == slot, takes[slot], device)
        assign[device * 2 + before] = jnp.int32(s)


def neighbours_of(assign, owners, places, device):
    found = []
    for j in range(2 * NEIGHBOURS):
        span = assign[device * 2 + j // NEIGHBOURS]
        found.append((owners[j % NEIGHBOURS, span], places[j % NEIGHBOURS, span]))
    return found


def pick_kernel(assign, owners, places, store, *rest):
    outs, (buf, sem_in, sem_out) = rest[:3], rest[3:]
    me = head_index()
    most = outs[0].shape[0]
    ins, puts = [], []
    for i in range(3):
        slots = [jnp.int32(0)] * most
        count = jnp.int32(0)
        for owner, place in neighbours_of(assign, owners, places, me ^ (i + 1)):
            here = owner == me
            for c in range(most):
                slots[c] = jnp.where(here & (count == c), place, slots[c])
            count = count + here.astype(jnp.int32)
        for c in range(most):
            k = i * most + c
            ins.append(pltpu.make_async_copy(store.at[slots[c]], buf.at[k], sem_in.at[k]))
            puts.append(pltpu.make_async_copy(buf.at[k], outs[i].at[c], sem_out.at[k]))
            ins[-1].start()
    for get, put in zip(ins, puts):
        get.wait()
        put.start()
    for c in puts:
        c.wait()


def context_kernel(assign, x, w, *rest):
    outs, buf = rest[:4], rest[4]
    me = head_index()
    width = w.shape[1]
    half = width // 2
    for c in range(2):
        cols = slice(c * half, (c + 1) * half)
        buf[:, cols] = dot(x[...], w[:, cols]).astype(jnp.bfloat16)
    for k in range(4):
        for i in range(2):
            start = pl.multiple_of(assign[(me ^ k) * 2 + i] * SPAN_LEN, SPAN_LEN)
            outs[k][i * SPAN_LEN : (i + 1) * SPAN_LEN, :] = buf[pl.ds(start, SPAN_LEN), :]


def load_pieces(n_span, pieces, held, sems):
    z = lax.axis_index("span").astype(jnp.int32)
    g = lax.axis_index("group").astype(jnp.int32)
    rows = pieces[0].shape[0]
    copies = []
    for i, piece in enumerate(pieces):
        spot = lax.rem(z + (n_span - i // 2), n_span) * 2 + (g ^ (i % 2))
        start = pl.multiple_of(spot * rows, rows)
        copies.append(
            pltpu.make_async_copy(piece, held.at[pl.ds(start, rows), :], sems.at[i])
        )
    return copies


def self_kernel(n_span, assign, owners, places, store, r1, r2, r3, *rest):
    pieces = rest[: 2 * n_span]
    source, within, held, triple, scores, weights, sem_s, sem_w = rest[2 * n_span :]
    me = head_index()
    per = 2 * NEIGHBOURS
    copies = load_pieces(n_span, pieces, held, sem_w)
    mine = neighbours_of(assign, owners, places, me)
    for j, (owner, place) in enumerate(mine):
        at = source.at[pl.ds(j * RETRIEVED, RETRIEVED), :]
        relation = owner ^ me
        nth = sum(((mine[t][0] == owner).astype(jnp.int32) for t in range(j)), jnp.int32(0))
        nth = jnp.minimum(nth, r1.shape[0] - 1)
        for k, ref in enumerate((store, r1, r2, r3)):

            @pl.when(relation == k)
            def _():
                pltpu.make_async_copy(ref.at[place if k == 0 else nth], at, sem_s.at[j]).start()

    for c in copies:
        c.start()
    for j in range(per):
        at = source.at[pl.ds(j * RETRIEVED, RETRIEVED), :]
        pltpu.make_async_copy(r1.at[0], at, sem_s.at[j]).wait()
    for c in copies:
        c.wait()
    breadth = source.shape[1]
    for c in range(3):
        cols = slice(c * breadth, (c + 1) * breadth)
        triple[:, cols] = dot(source[...], held[:, cols]).astype(jnp.bfloat16)
    units = []
    for j in range(per):
        rows = slice(j * RETRIEVED, (j + 1) * RETRIEVED)
        for c in range(0, breadth, HEAD_DIM):
            units.append(unit(triple, rows, c, triple, rows, breadth + c, 2 * breadth + c, within))
    attend_many(units, scores, weights)


def cross_kernel(n_span, source, within, c0, c1, c2, c3, *rest):
    pieces = rest[: 2 * n_span]
    outs = rest[2 * n_span : -8]
    held, context, middle, asking, across, scores, weights, sem_w = rest[-8:]
    copies = load_pieces(n_span, pieces, held, sem_w)
    for c in copies:
        c.start()
    breadth = source.shape[1]
    total = c0[...].astype(jnp.float32) + c1[...].astype(jnp.float32)
    total = total + (c2[...].astype(jnp.float32) + c3[...].astype(jnp.float32))
    context[...] = total.astype(jnp.bfloat16)
    for c in copies:
        c.wait()
    middle[...] = (
        source[...].astype(jnp.float32) + dot(within[...], held[:, :breadth])
    ).astype(jnp.bfloat16)
    asking[...] = dot(middle[...], held[:, breadth : 2 * breadth]).astype(jnp.bfloat16)
    span_rows = NEIGHBOURS * RETRIEVED
    units = []
    for s in range(len(outs)):
        rows = slice(s * span_rows, (s + 1) * span_rows)
        keys = slice(s * SPAN_LEN, (s + 1) * SPAN_LEN)
        for c in range(0, breadth, HEAD_DIM):
            units.append(unit(asking, rows, c, context, keys, c, breadth + c, across))
    attend_many(units, scores, weights)
    for s, out in enumerate(outs):
        rows = slice(s * span_rows, (s + 1) * span_rows)
        out[...] = (
            middle[rows, :].astype(jnp.float32) + dot(across[rows, :], held[:, 2 * breadth :])
        ).astype(jnp.bfloat16)


def query_kernel(own, x0, x1, y0, y1, d0, d1, w, out, held, total, sems):
    me = head_index()
    width = own.shape[1]
    half = x0.shape[0]
    copies = []
    for k in range(4):
        start = pl.multiple_of((me ^ k) * width, width)
        copies.append(
            pltpu.make_async_copy(w.at[pl.ds(start, width), :], held.at[k], sems.at[k])
        )
    for c in copies:
        c.start()
    copies[0].wait()
    total[...] = dot(own[...], held[0])
    for k, (a, b) in enumerate(((x0, x1), (y0, y1), (d0, d1))):
        copies[k + 1].wait()
        total[:half, :] += dot(a[...], held[k + 1])
        total[half:, :] += dot(b[...], held[k + 1])
    out[...] = total[...].astype(jnp.bfloat16)


def span_kernel(relations, assign, queries, *rest):
    n = 2 * len(relations)
    encs = rest[:n]
    pair, held = rest[n : n + 2]
    outs = rest[n + 2 : n + 6]
    q, keep, memory, att, scores, weights, sem = rest[n + 6 :]
    me = head_index()
    local = q.shape[1]
    span_rows = NEIGHBOURS * RETRIEVED
    loads = []
    for i in range(n):
        span = assign[(me ^ relations[i // 2]) * 2 + i % 2]
        at = pl.ds(pl.multiple_of(span * SPAN_LEN, SPAN_LEN), SPAN_LEN)
        to_rows = pl.ds(i * SPAN_LEN, SPAN_LEN)
        loads.append(pltpu.make_async_copy(queries.at[at, :], q.at[to_rows, :], sem.at[i]))
    for c in loads:
        c.start()
    for s in range(n):
        keep[s * span_rows : (s + 1) * span_rows, :] = encs[s][...]
    for c in range(2):
        cols = slice(c * local, (c + 1) * local)
        memory[:, cols] = dot(keep[...], pair[:, cols]).astype(jnp.bfloat16)
    for c in loads:
        c.wait()
    units = []
    for s in range(n):
        r = slice(s * SPAN_LEN, (s + 1) * SPAN_LEN)
        m = slice(s * span_rows, (s + 1) * span_rows)
        for c in range(0, local, HEAD_DIM):
            units.append(unit(q, r, c, memory, m, c, local + c, att))
    attend_many(units, scores, weights)
    width = outs[0].shape[1]
    for k in range(4):
        start = pl.multiple_of((me ^ k) * width, width)
        outs[k][...] = dot(att[...], held[:, pl.ds(start, width)]).astype(jnp.bfloat16)


def final_kernel(assign, states, *rest):
    terms, out = rest[:12], rest[12]
    me = head_index()
    chunk_of = ((0, 0), (1, 0), (1, 1), (2, 0))
    for m, i in ((m, i) for m in range(4) for i in range(2)):
        span = assign[(me ^ m) * 2 + i]
        at = pl.ds(pl.multiple_of(span * SPAN_LEN, SPAN_LEN), SPAN_LEN)
        parts = []
        for k in range(4):
            chunk, part = chunk_of[k ^ m]
            start = (2 * part + i) * SPAN_LEN
            term = terms[4 * chunk + k][start : start + SPAN_LEN, :]
            parts.append(term.astype(jnp.float32))
        total = (parts[0] + parts[1]) + (parts[2] + parts[3])
        out[at, :] = (states[at, :].astype(jnp.float32) + total).astype(jnp.bfloat16)


def shape(*dims):
    return jax.ShapeDtypeStruct(dims, jnp.bfloat16)


def to(k, value):
    return lax.ppermute(value, "head", [(i, i ^ k) for i in range(4)])


def fast(
    n_span,
    states,
    owners,
    places,
    stored,
    encoder_weights,
    context_weight,
    query_weight,
    neighbour_weight,
    output_weight,
):
    bf16 = jnp.bfloat16
    tokens, feat = states.shape
    span_count = owners.shape[0]
    per = span_count * NEIGHBOURS // 4
    own_spans = span_count // 4
    local = query_weight.shape[1]
    store = stored.reshape(stored.shape[3], RETRIEVED, ENC_WIDTH)
    owners, places = owners.T, places.T

    table = jnp.asarray(pair_table(span_count))
    assign = pl.pallas_call(
        plan_kernel,
        out_shape=jax.ShapeDtypeStruct((span_count,), jnp.int32),
        in_specs=[SMEM, VMEM],
        out_specs=SMEM,
        name="plan",
    )(owners, table)

    most = 2
    sends = call(
        pick_kernel,
        [shape(most, RETRIEVED, ENC_WIDTH)] * 3,
        [SMEM] * 3 + [HBM],
        [HBM] * 3,
        [
            pltpu.VMEM((3 * most, RETRIEVED, ENC_WIDTH), bf16),
            pltpu.SemaphoreType.DMA((3 * most,)),
            pltpu.SemaphoreType.DMA((3 * most,)),
        ],
        8,
        4 * 10**9,
        assign,
        owners,
        places,
        store,
    )
    raw = [to(k + 1, sends[k]) for k in range(3)]

    cut = 3 * ENC_WIDTH
    ring = [(i, (i + 1) % n_span) for i in range(n_span)]
    halves = []
    for part in (encoder_weights[:, :cut], encoder_weights[:, cut:]):
        pieces, now = [], part
        for r in range(n_span):
            if r:
                now = lax.ppermute(now, "span", ring)
            pieces.append(now)
            pieces.append(lax.ppermute(now, "group", [(0, 1), (1, 0)]))
        halves.append(pieces)
    n_pieces = 2 * n_span

    width_c = context_weight.shape[1]
    rows_c = tokens // 4
    part_c = call(
        context_kernel,
        [shape(rows_c, width_c)] * 4,
        [SMEM, VMEM, VMEM],
        [VMEM] * 4,
        [pltpu.VMEM((tokens, width_c), bf16)],
        16,
        2 * tokens * feat * width_c,
        assign,
        states,
        context_weight,
    )
    context = [part_c[0]] + [to(k, part_c[k]) for k in range(1, 4)]

    half_t = tokens // 2
    s0, s1 = states[:half_t], states[half_t:]
    x0, y1 = to(1, s0), to(2, s1)
    x1, y0 = to(1, s1), to(2, s0)
    d0, d1 = to(2, x0), to(1, y1)

    source, within = call(
        functools.partial(self_kernel, n_span),
        [shape(per * RETRIEVED, ENC_WIDTH)] * 2,
        [SMEM] * 3 + [HBM] * (4 + n_pieces),
        [VMEM] * 2,
        [
            pltpu.VMEM((ENC_WIDTH, cut), bf16),
            pltpu.VMEM((per * RETRIEVED, cut), bf16),
            pltpu.VMEM((per * ENC_WIDTH, RETRIEVED), jnp.float32),
            pltpu.VMEM((per * ENC_WIDTH, RETRIEVED), bf16),
            pltpu.SemaphoreType.DMA((per,)),
            pltpu.SemaphoreType.DMA((n_pieces,)),
        ],
        20,
        4 * per * RETRIEVED * ENC_WIDTH * cut,
        assign,
        owners,
        places,
        store,
        *raw,
        *halves[0],
    )
    span_rows = NEIGHBOURS * RETRIEVED
    enc = call(
        functools.partial(cross_kernel, n_span),
        [shape(span_rows, ENC_WIDTH)] * own_spans,
        [VMEM] * 6 + [HBM] * n_pieces,
        [VMEM] * own_spans,
        [
            pltpu.VMEM((ENC_WIDTH, cut), bf16),
            pltpu.VMEM((rows_c, width_c), bf16),
            pltpu.VMEM((per * RETRIEVED, ENC_WIDTH), bf16),
            pltpu.VMEM((per * RETRIEVED, ENC_WIDTH), bf16),
            pltpu.VMEM((per * RETRIEVED, ENC_WIDTH), bf16),
            pltpu.VMEM((per * ENC_WIDTH, SPAN_LEN), jnp.float32),
            pltpu.VMEM((per * ENC_WIDTH, SPAN_LEN), bf16),
            pltpu.SemaphoreType.DMA((n_pieces,)),
        ],
        20,
        4 * per * RETRIEVED * ENC_WIDTH * cut,
        source,
        within,
        *context,
        *halves[1],
    )
    first = own_spans // 2
    x = [to(1, e) for e in enc]
    y = [to(2, e) for e in enc]
    d = [to(2, x[i]) for i in range(first)]
    d += [to(1, y[i]) for i in range(first, own_spans)]

    queries = call(
        query_kernel,
        shape(tokens, local),
        [VMEM] * 7 + [HBM],
        VMEM,
        [
            pltpu.VMEM((4, feat, local), bf16),
            pltpu.VMEM((tokens, local), jnp.float32),
            pltpu.SemaphoreType.DMA((4,)),
        ],
        24,
        8 * tokens * feat * local,
        states,
        x0,
        x1,
        y0,
        y1,
        d0,
        d1,
        query_weight,
    )
    w_pair = neighbour_weight.reshape(ENC_WIDTH, 2 * local)
    arrived = []
    for relations, chunk in (((0,), enc), ((1, 2), x + y), ((3,), d)):
        spans = len(chunk)
        rows = spans * SPAN_LEN
        terms = call(
            functools.partial(span_kernel, relations),
            [shape(rows, feat)] * 4,
            [SMEM, HBM] + [VMEM] * (spans + 2),
            [VMEM] * 4,
            [
                pltpu.VMEM((rows, local), bf16),
                pltpu.VMEM((spans * span_rows, ENC_WIDTH), bf16),
                pltpu.VMEM((spans * span_rows, 2 * local), bf16),
                pltpu.VMEM((rows, local), bf16),
                pltpu.VMEM((rows * local // HEAD_DIM, span_rows), jnp.float32),
                pltpu.VMEM((rows * local // HEAD_DIM, span_rows), bf16),
                pltpu.SemaphoreType.DMA((spans,)),
            ],
            32,
            4 * spans * span_rows * ENC_WIDTH * 2 * local,
            assign,
            queries,
            *chunk,
            w_pair,
            output_weight,
        )
        arrived.append(terms[0])
        arrived += [to(k, terms[k]) for k in range(1, 4)]
    return call(
        final_kernel,
        shape(tokens, feat),
        [SMEM] + [VMEM] * 13,
        VMEM,
        [],
        16,
        17 * tokens * feat,
        assign,
        states,
        *arrived,
    )


def solution(mesh):
    sizes = mesh.shape
    n_head, n_span = sizes["head"], sizes["span"]
    square = n_head == 4 and sizes["group"] == 2

    def per_device(*args):
        spans = args[1].shape[0]
        if square and spans == 2 * n_head:
            return fast(n_span, *args)
        return general(*args)

    in_specs = (
        P(("span", "group"), "head"),
        P(("span", "group"), None),
        P(("span", "group"), None),
        P("span", "head", "group", None, None, None),
        P(("span", "group"), None),
        P("head", None),
        P(None, "head"),
        P(None, None, "head"),
        P("head", None),
    )
    out_specs = P(("span", "group"), "head")
    return jax.shard_map(
        per_device, mesh=mesh, in_specs=in_specs, out_specs=out_specs, check_vma=False
    )
```

```python
import functools

import jax
import jax.numpy as jnp
import numpy as np
from jax import lax
from jax.experimental import pallas as pl
from jax.experimental.pallas import tpu as pltpu
from jax.sharding import PartitionSpec as P


HEAD_DIM = 128
ENC_WIDTH = 896
SPAN_LEN = 64
RETRIEVED = 128
NEIGHBOURS = 2


HBM = pl.BlockSpec(memory_space=pltpu.HBM)
VMEM = pl.BlockSpec(memory_space=pltpu.VMEM)
SMEM = pl.BlockSpec(memory_space=pltpu.SMEM)


def attend(queries, keys_in, values_in, factor):
    scores = (
        jnp.einsum("bqhe,bkhe->bhqk", queries, keys_in, preferred_element_type=jnp.float32) * factor
    )
    weights = jax.nn.softmax(scores, axis=-1).astype(jnp.bfloat16)
    result = jnp.einsum("bhqk,bkhe->bqhe", weights, values_in, preferred_element_type=jnp.float32)
    return result.astype(jnp.bfloat16)


def encode(source, context, weights):
    number, length, breadth = source.shape
    groups = breadth // HEAD_DIM
    factor = HEAD_DIM ** (-0.5)
    rows_in = source.reshape(number * length, breadth)
    triple = jnp.dot(rows_in, weights[:, : 3 * breadth], preferred_element_type=jnp.float32).astype(
        jnp.bfloat16
    )
    triple = triple.reshape(number, length, 3, groups, HEAD_DIM)
    within = attend(triple[:, :, 0], triple[:, :, 1], triple[:, :, 2], factor).reshape(
        number * length, breadth
    )
    middle = rows_in.astype(jnp.float32) + jnp.dot(
        within, weights[:, 3 * breadth : 4 * breadth], preferred_element_type=jnp.float32
    )
    middle = middle.astype(jnp.bfloat16)
    asking = jnp.dot(
        middle, weights[:, 4 * breadth : 5 * breadth], preferred_element_type=jnp.float32
    ).astype(jnp.bfloat16)
    asking = asking.reshape(number, length, groups, HEAD_DIM)
    paired = context.reshape(number, context.shape[1], 2, groups, HEAD_DIM)
    across = attend(asking, paired[:, :, 0], paired[:, :, 1], factor).reshape(
        number * length, breadth
    )
    result = middle.astype(jnp.float32) + jnp.dot(
        across, weights[:, 5 * breadth :], preferred_element_type=jnp.float32
    )
    return result.astype(jnp.bfloat16).reshape(number, length, breadth)


def general(
    states,
    owners,
    places,
    stored,
    encoder_weights,
    context_weight,
    query_weight,
    neighbour_weight,
    output_weight,
):
    position = lax.axis_index("head")
    token_rows = states.shape[0]
    span_count = owners.shape[0]
    pair_count = span_count * NEIGHBOURS
    local_width = query_weight.shape[1]
    local_heads = local_width // HEAD_DIM
    factor = HEAD_DIM ** (-0.5)
    query_sums = jnp.dot(
        lax.all_gather(states, "head", axis=1, tiled=True),
        query_weight,
        preferred_element_type=jnp.float32,
    )
    queries = query_sums.astype(jnp.bfloat16)
    partial_context = jnp.dot(states, context_weight, preferred_element_type=jnp.float32)
    context = lax.psum(partial_context.astype(jnp.bfloat16), "head")
    context = context.reshape(span_count, SPAN_LEN, 2 * ENC_WIDTH)
    weights_all = lax.all_gather(encoder_weights, ("span", "group"), axis=0, tiled=True)
    owner_flat = owners.reshape(pair_count)
    place_flat = places.reshape(pair_count)
    pair_ids = jnp.arange(pair_count, dtype=jnp.int32)
    local_store = stored.reshape(stored.shape[3], stored.shape[4], stored.shape[5])
    slot_count = local_store.shape[0]
    slot_ids = jnp.arange(slot_count, dtype=jnp.int32)
    matched = (owner_flat[None, :] == position) & (place_flat[None, :] == slot_ids[:, None])
    span_of = jnp.sum(jnp.where(matched, pair_ids[None, :] // NEIGHBOURS, 0), axis=1)
    encoded = encode(local_store, context[span_of], weights_all)
    local_pair = neighbour_weight.reshape(ENC_WIDTH, 2 * local_width)
    piece = lax.all_gather(encoded, "head", axis=0, tiled=True)
    rows_in = piece.reshape(piece.shape[0] * RETRIEVED, ENC_WIDTH)
    result = jnp.dot(rows_in, local_pair, preferred_element_type=jnp.float32).astype(jnp.bfloat16)
    gathered = result.reshape(piece.shape[0], RETRIEVED, 2 * local_width)
    neighbour_pairs = gathered[owner_flat * slot_count + place_flat]
    asked = queries.reshape(span_count, SPAN_LEN, local_heads, HEAD_DIM)
    memory = neighbour_pairs.reshape(span_count, NEIGHBOURS * RETRIEVED, 2, local_heads, HEAD_DIM)
    attended = attend(asked, memory[:, :, 0], memory[:, :, 1], factor).reshape(
        token_rows, local_width
    )
    terms = jnp.dot(attended, output_weight, preferred_element_type=jnp.float32)
    summed = lax.psum_scatter(
        terms.astype(jnp.bfloat16), "head", scatter_dimension=1, tiled=True
    ).astype(jnp.float32)
    return (states.astype(jnp.float32) + summed).astype(jnp.bfloat16)


def call(kernel, out_shape, in_specs, out_specs, scratch, mib, flops, *args):
    return pl.pallas_call(
        kernel,
        out_shape=out_shape,
        in_specs=in_specs,
        out_specs=out_specs,
        scratch_shapes=scratch,
        compiler_params=pltpu.CompilerParams(vmem_limit_bytes=mib * 1024 * 1024),
        cost_estimate=pl.CostEstimate(
            flops=flops,
            bytes_accessed=2 * sum(a.size for a in args),
            transcendentals=0,
        ),
    )(*args)


def dot(a, b):
    return jnp.dot(a, b, preferred_element_type=jnp.float32)


def attend_many(units, scores, weights):
    rows = scores.shape[0] // len(units)
    part = [slice(i * rows, (i + 1) * rows) for i in range(len(units))]
    factor = HEAD_DIM ** (-0.5)
    for at, (q, k, _, _) in zip(part, units):
        scores[at, :] = lax.dot_general(
            q(), k(), (((1,), (1,)), ((), ())), preferred_element_type=jnp.float32
        )
    for at in part:
        one = scores[at, :]
        top = jnp.max(one, axis=-1, keepdims=True)
        weights[at, :] = jnp.exp((one - top) * factor).astype(jnp.bfloat16)
    for at, (_, _, v, put) in zip(part, units):
        values = v()
        both = dot(weights[at, :], jnp.concatenate([values, jnp.ones_like(values)], axis=1))
        put((both[:, :HEAD_DIM] / both[:, HEAD_DIM:]).astype(jnp.bfloat16))


def unit(q, q_rows, q_col, k, k_rows, k_col, v_col, out):
    def put(value):
        out[q_rows, q_col : q_col + HEAD_DIM] = value

    return (
        lambda: q[q_rows, q_col : q_col + HEAD_DIM],
        lambda: k[k_rows, k_col : k_col + HEAD_DIM],
        lambda: k[k_rows, v_col : v_col + HEAD_DIM],
        put,
    )


def head_index():
    return lax.axis_index("head").astype(jnp.int32)


def square_place():
    me = head_index()
    return me % 2, me // 2


def cut_kernel(weights, query_part, half_part, last_part, sems):
    _, y = square_place()
    width = half_part.shape[1]
    first = query_part.shape[1]
    copies = []
    for i, (start, part) in enumerate(
        ((0, query_part), (first + y * width, half_part), (first + 2 * width, last_part))
    ):
        cols = pl.ds(pl.multiple_of(start, HEAD_DIM), part.shape[1])
        copies.append(pltpu.make_async_copy(weights.at[:, cols], part, sems.at[i]))
    for c in copies:
        c.start()
    for c in copies:
        c.wait()


def pairings(items):
    if not items:
        yield ()
        return
    for other in items[1:]:
        rest = tuple(i for i in items[1:] if i != other)
        for more in pairings(rest):
            yield ((items[0], other),) + more


def pair_table(spans):
    every = list(pairings(tuple(range(spans))))
    table = np.full((spans, -(-len(every) // 128) * 128), -1, np.int32)
    for c, pairing in enumerate(every):
        for slot, pair in enumerate(pairing):
            for span in pair:
                table[span, c] = slot
    return table


def plan_kernel(owners, table, assign):
    spans = table.shape[0]
    devices = spans // 2
    shape_row = (1, table.shape[1])
    hits = [
        [sum((owners[n, s] == o).astype(jnp.int32) for n in range(NEIGHBOURS)) for s in range(spans)]
        for o in range(devices)
    ]
    rows = [table[s : s + 1, :] for s in range(spans)]
    inside = [[(r == slot).astype(jnp.int32) for r in rows] for slot in range(devices)]
    fits = rows[0] >= 0
    for o in range(devices):
        heavy = jnp.zeros(shape_row, jnp.int32)
        for slot in range(devices):
            count = jnp.zeros(shape_row, jnp.int32)
            for s in range(spans):
                count = count + inside[slot][s] * hits[o][s]
            heavy = heavy + (count >= 3).astype(jnp.int32)
        fits = fits & (heavy <= 1)
    code = jnp.zeros(shape_row, jnp.int32)
    for s in range(spans):
        code = code + rows[s] * (devices**s)
    worst = devices**spans
    chosen = jnp.min(jnp.where(fits, code, worst).astype(jnp.float32)).astype(jnp.int32)
    slot_of = []
    for s in range(spans):
        slot_of.append(lax.rem(chosen, devices))
        chosen = lax.div(chosen, devices)
    takes = []
    for slot in range(devices):
        taker = jnp.int32(-1)
        for o in range(devices):
            count = sum(jnp.where(slot_of[s] == slot, hits[o][s], 0) for s in range(spans))
            taker = jnp.where(count >= 3, o, taker)
        takes.append(taker)
    for slot in range(devices):
        free = jnp.int32(0)
        for d in reversed(range(devices)):
            taken = sum((t == d).astype(jnp.int32) for t in takes)
            free = jnp.where(taken == 0, d, free)
        takes[slot] = jnp.where(takes[slot] < 0, free, takes[slot])
    for s in range(spans):
        before = sum(((slot_of[t] == slot_of[s]).astype(jnp.int32) for t in range(s)), jnp.int32(0))
        device = jnp.int32(0)
        for slot in range(devices):
            device = jnp.where(slot_of[s] == slot, takes[slot], device)
        assign[device * 2 + before] = jnp.int32(s)


def neighbours_of(assign, owners, places, device):
    found = []
    for j in range(2 * NEIGHBOURS):
        span = assign[device * 2 + j // NEIGHBOURS]
        found.append((owners[j % NEIGHBOURS, span], places[j % NEIGHBOURS, span]))
    return found


def pick_kernel(assign, owners, places, store, *rest):
    outs, (buf, sem_in, sem_out) = rest[:3], rest[3:]
    me = head_index()
    most = outs[0].shape[0]
    ins, puts = [], []
    for i in range(3):
        slots = [jnp.int32(0)] * most
        count = jnp.int32(0)
        for owner, place in neighbours_of(assign, owners, places, me ^ (i + 1)):
            here = owner == me
            for c in range(most):
                slots[c] = jnp.where(here & (count == c), place, slots[c])
            count = count + here.astype(jnp.int32)
        for c in range(most):
            k = i * most + c
            ins.append(pltpu.make_async_copy(store.at[slots[c]], buf.at[k], sem_in.at[k]))
            puts.append(pltpu.make_async_copy(buf.at[k], outs[i].at[c], sem_out.at[k]))
            ins[-1].start()
    for get, put in zip(ins, puts):
        get.wait()
        put.start()
    for c in puts:
        c.wait()


def context_kernel(assign, x, w, own, to_x, to_y, for_y, for_x, buf, sems):
    me = head_index()
    width = w.shape[1]
    half = width // 2
    for c in range(2):
        cols = slice(c * half, (c + 1) * half)
        buf[:, cols] = dot(x[...], w[:, cols]).astype(jnp.bfloat16)
    copies = []
    for out, parts in (
        (to_x, ((1, 0), (3, 0))),
        (to_y, ((2, 1), (3, 1))),
        (for_y, ((2, 0),)),
        (for_x, ((1, 1),)),
        (own, ((0, 0), (0, 1))),
    ):
        for n, (k, i) in enumerate(parts):
            start = pl.multiple_of(assign[(me ^ k) * 2 + i] * SPAN_LEN, SPAN_LEN)
            rows = out.at[pl.ds(n * SPAN_LEN, SPAN_LEN), :]
            part = buf.at[pl.ds(start, SPAN_LEN), :]
            copies.append(pltpu.make_async_copy(part, rows, sems.at[len(copies)]))
            copies[-1].start()
    for c in copies:
        c.wait()


def load_pieces(n_span, first, pieces, held, sems):
    z = lax.axis_index("span").astype(jnp.int32)
    g = lax.axis_index("group").astype(jnp.int32)
    x, y = square_place()
    rows = pieces[0].shape[0]
    copies = []
    split = (len(pieces) - 2) // (2 * (n_span - 1))
    for i, piece in enumerate(pieces):
        if i < 2:
            r, other, cols = 0, i, slice(None)
            piece = piece.at[:, pl.ds(first, held.shape[1])]
        else:
            r, rest = 1 + (i - 2) // (2 * split), (i - 2) % (2 * split)
            other = rest % 2
            cols = slice(None)
            if split == 2:
                place = y if half_axis(n_span, r) else x
                block = place if rest < 2 else 1 - place
                width = held.shape[1] // 2
                cols = pl.ds(pl.multiple_of(block * width, width), width)
        spot = lax.rem(z + (n_span - r), n_span) * 2 + (g ^ other)
        start = pl.multiple_of(spot * rows, rows)
        copies.append(
            pltpu.make_async_copy(piece, held.at[pl.ds(start, rows), cols], sems.at[i])
        )
    return copies


def half_axis(n_span, r):
    return min(r, n_span - 2) % 2


def self_kernel(n_span, assign, owners, places, store, r1, r2, r3, *rest):
    pieces = rest[: 2 * n_span]
    source, within, held, triple, scores, weights, sem_s, sem_w = rest[2 * n_span :]
    me = head_index()
    per = 2 * NEIGHBOURS
    copies = load_pieces(n_span, 0, pieces, held, sem_w)
    mine = neighbours_of(assign, owners, places, me)
    for j, (owner, place) in enumerate(mine):
        at = source.at[pl.ds(j * RETRIEVED, RETRIEVED), :]
        relation = owner ^ me
        nth = sum(((mine[t][0] == owner).astype(jnp.int32) for t in range(j)), jnp.int32(0))
        nth = jnp.minimum(nth, r1.shape[0] - 1)
        for k, ref in enumerate((store, r1, r2, r3)):

            @pl.when(relation == k)
            def _():
                pltpu.make_async_copy(ref.at[place if k == 0 else nth], at, sem_s.at[j]).start()

    for c in copies:
        c.start()
    for j in range(per):
        at = source.at[pl.ds(j * RETRIEVED, RETRIEVED), :]
        pltpu.make_async_copy(r1.at[0], at, sem_s.at[j]).wait()
    for c in copies:
        c.wait()
    breadth = source.shape[1]
    for c in range(3):
        cols = slice(c * breadth, (c + 1) * breadth)
        triple[:, cols] = dot(source[...], held[:, cols]).astype(jnp.bfloat16)
    units = []
    for j in range(per):
        rows = slice(j * RETRIEVED, (j + 1) * RETRIEVED)
        for c in range(0, breadth, HEAD_DIM):
            units.append(unit(triple, rows, c, triple, rows, breadth + c, 2 * breadth + c, within))
    attend_many(units, scores, weights)


def cross_kernel(n_span, first, source, within, own, from_x, from_y, last_y, last_x, *rest):
    pieces = rest[: 4 * n_span - 2]
    middle, across, held, context, asking, scores, weights, sem_w = rest[4 * n_span - 2 :]
    copies = load_pieces(n_span, first, pieces, held, sem_w)
    for c in copies:
        c.start()
    breadth = source.shape[1]
    for i, (near, far) in enumerate(((from_x, last_y), (from_y, last_x))):
        at = slice(i * SPAN_LEN, (i + 1) * SPAN_LEN)
        total = own[at, :].astype(jnp.float32) + near[:SPAN_LEN, :].astype(jnp.float32)
        context[at, :] = (total + far[...].astype(jnp.float32)).astype(jnp.bfloat16)
    for c in copies:
        c.wait()
    middle[...] = (
        source[...].astype(jnp.float32) + dot(within[...], held[:, :breadth])
    ).astype(jnp.bfloat16)
    asking[...] = dot(middle[...], held[:, breadth:]).astype(jnp.bfloat16)
    span_rows = NEIGHBOURS * RETRIEVED
    units = []
    for s in range(2):
        rows = slice(s * span_rows, (s + 1) * span_rows)
        keys = slice(s * SPAN_LEN, (s + 1) * SPAN_LEN)
        for c in range(0, breadth, HEAD_DIM):
            units.append(unit(asking, rows, c, context, keys, c, breadth + c, across))
    attend_many(units, scores, weights)


def encoded_kernel(n_span, first, middle, across, *rest):
    pieces = rest[: 2 * n_span]
    outs, held, sem_w = rest[2 * n_span : -2], rest[-2], rest[-1]
    copies = load_pieces(n_span, first, pieces, held, sem_w)
    for c in copies:
        c.start()
    for c in copies:
        c.wait()
    span_rows = NEIGHBOURS * RETRIEVED
    total = middle[...].astype(jnp.float32) + dot(across[...], held[...])
    for s, out in enumerate(outs):
        out[...] = total[s * span_rows : (s + 1) * span_rows, :].astype(jnp.bfloat16)


def query_kernel(own, from_x, from_y, d0, d1, w, out, held, total, sems):
    me = head_index()
    width = own.shape[1]
    half = d0.shape[0]
    copies = []
    for k in range(4):
        start = pl.multiple_of((me ^ k) * width, width)
        copies.append(
            pltpu.make_async_copy(w.at[pl.ds(start, width), :], held.at[k], sems.at[k])
        )
    for c in copies:
        c.start()
    copies[0].wait()
    total[...] = dot(own[...], held[0])
    for k, from_k in enumerate((from_x, from_y)):
        copies[k + 1].wait()
        total[...] += dot(from_k[...], held[k + 1])
    copies[3].wait()
    total[:half, :] += dot(d0[...], held[3])
    total[half:, :] += dot(d1[...], held[3])
    out[...] = total[...].astype(jnp.bfloat16)


CHUNKS = (((0, 0), (1, 0), (0, 1), (2, 1)), ((2, 0), (3, 0), (1, 1), (3, 1)))


def attend_spans(spans, assign, queries, encs, pair, att, rows_of, scratch):
    q, keep, memory, scores, weights, sem = scratch
    me = head_index()
    local = q.shape[1]
    span_rows = NEIGHBOURS * RETRIEVED
    loads = []
    for s, (relation, i) in enumerate(spans):
        span = assign[(me ^ relation) * 2 + i]
        at = pl.ds(pl.multiple_of(span * SPAN_LEN, SPAN_LEN), SPAN_LEN)
        to_rows = pl.ds(rows_of[s] * SPAN_LEN, SPAN_LEN)
        loads.append(pltpu.make_async_copy(queries.at[at, :], q.at[to_rows, :], sem.at[s]))
    for c in loads:
        c.start()
    for s in range(len(spans)):
        keep[s * span_rows : (s + 1) * span_rows, :] = encs[s][...]
    for c in range(2):
        cols = slice(c * local, (c + 1) * local)
        memory[:, cols] = dot(keep[...], pair[:, cols]).astype(jnp.bfloat16)
    for c in loads:
        c.wait()
    units = []
    for s in range(len(spans)):
        r = slice(rows_of[s] * SPAN_LEN, (rows_of[s] + 1) * SPAN_LEN)
        m = slice(s * span_rows, (s + 1) * span_rows)
        for c in range(0, local, HEAD_DIM):
            units.append(unit(q, r, c, memory, m, c, local + c, att))
    attend_many(units, scores, weights)


def early_kernel(spans, assign, queries, *rest):
    n = len(spans)
    attend_spans(spans, assign, queries, rest[:n], rest[n], rest[n + 1], range(n), rest[n + 2 :])


def span_kernel(chunk, early, assign, queries, *rest):
    late = [s for s in range(len(chunk)) if s not in early]
    n = len(late)
    encs, rest = rest[:n], rest[n:]
    if early:
        before, rest = rest[0], rest[1:]
    pair, held, keep_a, keep_b, to_x, to_y, att = rest[:7]
    me = head_index()
    for i, s in enumerate(early):
        att[s * SPAN_LEN : (s + 1) * SPAN_LEN, :] = before[i * SPAN_LEN : (i + 1) * SPAN_LEN, :]
    attend_spans([chunk[s] for s in late], assign, queries, encs, pair, att, late, rest[7:])
    width = keep_a.shape[1] // 2
    one = SPAN_LEN
    low, high = slice(0, width), slice(width, 2 * width)
    places = (
        ((keep_a, low, False), (keep_b, low, False)),
        ((to_x, low, True), (keep_b, high, False)),
        ((keep_a, high, False), (to_y, low, True)),
        ((to_x, high, True), (to_y, high, True)),
    )
    for k in range(4):
        start = pl.multiple_of((me ^ k) * width, width)
        term = dot(att[...], held[:, pl.ds(start, width)]).astype(jnp.bfloat16)
        for side, (out, cols, swapped) in enumerate(places[k]):
            first = term[2 * side * one : (2 * side + 1) * one, :]
            second = term[(2 * side + 1) * one : (2 * side + 2) * one, :]
            out[:one, cols] = second if swapped else first
            out[one:, cols] = first if swapped else second


def final_kernel(assign, states, *rest):
    terms, out = rest[:-1], rest[-1]
    me = head_index()
    width = out.shape[1]
    for c, chunk in enumerate(CHUNKS):
        for s, (relation, i) in enumerate(chunk):
            side, row = s // 2, (s % 2) * SPAN_LEN
            near = slice(row, row + SPAN_LEN)
            span = assign[(me ^ relation) * 2 + i]
            at = pl.ds(pl.multiple_of(span * SPAN_LEN, SPAN_LEN), SPAN_LEN)
            kept, arrived = terms[6 * c + side], terms[6 * c + 2 + side]
            last = terms[6 * (1 - c) + 4 + side]
            total = kept[near, :width].astype(jnp.float32)
            total = total + arrived[near, :width].astype(jnp.float32)
            total = total + last[near, :].astype(jnp.float32)
            out[at, :] = (states[at, :].astype(jnp.float32) + total).astype(jnp.bfloat16)


def shape(*dims):
    return jax.ShapeDtypeStruct(dims, jnp.bfloat16)


def add(a, b):
    return (a.astype(jnp.float32) + b.astype(jnp.float32)).astype(jnp.bfloat16)


def to(k, value):
    return lax.ppermute(value, "head", [(i, i ^ k) for i in range(4)])


def fast(
    n_span,
    states,
    owners,
    places,
    stored,
    encoder_weights,
    context_weight,
    query_weight,
    neighbour_weight,
    output_weight,
):
    bf16 = jnp.bfloat16
    tokens, feat = states.shape
    span_count = owners.shape[0]
    per = span_count * NEIGHBOURS // 4
    own_spans = span_count // 4
    local = query_weight.shape[1]
    store = stored.reshape(stored.shape[3], RETRIEVED, ENC_WIDTH)
    owners, slots = owners.T, places.T

    starts = (0, 3 * ENC_WIDTH, 5 * ENC_WIDTH)
    widths = (3 * ENC_WIDTH, 2 * ENC_WIDTH, ENC_WIDTH)
    rows_w = encoder_weights.shape[0]
    cut = call(
        cut_kernel,
        [shape(rows_w, widths[0]), shape(rows_w, ENC_WIDTH), shape(rows_w, ENC_WIDTH)],
        [HBM],
        [VMEM] * 3,
        [pltpu.SemaphoreType.DMA((3,))],
        8,
        2 * 10**9,
        encoder_weights,
    )
    h = lax.axis_index("head")
    places = (h % 2, h // 2)

    def ring(value):
        return lax.ppermute(value, "span", [(i, (i + 1) % n_span) for i in range(n_span)])

    def swap(value):
        return lax.ppermute(value, "group", [(0, 1), (1, 0)])

    partner = swap(encoder_weights)
    parts = [[encoder_weights, partner] for _ in starts]
    whole, near, last = cut
    far = None
    for r in range(1, n_span):
        whole = ring(whole)
        if r < n_span - 1:
            if r > 1:
                same = places[half_axis(n_span, r)] == places[half_axis(n_span, r - 1)]
                near = jnp.where(same, near, far)
            near = ring(near)
            far = to(1 + half_axis(n_span, r), near)
        else:
            near, far = ring(near), ring(far)
        last = ring(last)
        parts[0] += [whole, swap(whole)]
        parts[1] += [near, swap(near), far, swap(far)]
        parts[2] += [last, swap(last)]
    n_pieces = [len(p) for p in parts]

    table = jnp.asarray(pair_table(span_count))
    assign = pl.pallas_call(
        plan_kernel,
        out_shape=jax.ShapeDtypeStruct((span_count,), jnp.int32),
        in_specs=[SMEM, VMEM],
        out_specs=SMEM,
        name="plan",
    )(owners, table)

    most = 2
    sends = call(
        pick_kernel,
        [shape(most, RETRIEVED, ENC_WIDTH)] * 3,
        [SMEM] * 3 + [HBM],
        [HBM] * 3,
        [
            pltpu.VMEM((3 * most, RETRIEVED, ENC_WIDTH), bf16),
            pltpu.SemaphoreType.DMA((3 * most,)),
            pltpu.SemaphoreType.DMA((3 * most,)),
        ],
        8,
        4 * 10**9,
        assign,
        owners,
        slots,
        store,
    )
    raw = [to(k + 1, sends[k]) for k in range(3)]

    width_c = context_weight.shape[1]
    rows_c = own_spans * SPAN_LEN
    own_c, to_x, to_y, for_y, for_x = call(
        context_kernel,
        [shape(rows_c, width_c)] * 3 + [shape(SPAN_LEN, width_c)] * 2,
        [SMEM, VMEM, VMEM],
        [HBM] * 5,
        [pltpu.VMEM((tokens, width_c), bf16), pltpu.SemaphoreType.DMA((8,))],
        16,
        2 * tokens * feat * width_c,
        assign,
        states,
        context_weight,
    )
    from_x, from_y = to(1, to_x), to(2, to_y)
    last_y = add(for_y, from_x[SPAN_LEN:])
    last_x = add(for_x, from_y[SPAN_LEN:])
    last_y, last_x = to(2, last_y), to(1, last_x)
    context = [own_c, from_x, from_y, last_y, last_x]

    half_t = tokens // 2
    states_x, states_y = to(1, states), to(2, states)
    d0, d1 = to(2, states_x[:half_t]), to(1, states_y[half_t:])

    source, within = call(
        functools.partial(self_kernel, n_span),
        [shape(per * RETRIEVED, ENC_WIDTH)] * 2,
        [SMEM] * 3 + [HBM] * (4 + n_pieces[0]),
        [VMEM] * 2,
        [
            pltpu.VMEM((ENC_WIDTH, widths[0]), bf16),
            pltpu.VMEM((per * RETRIEVED, widths[0]), bf16),
            pltpu.VMEM((per * ENC_WIDTH, RETRIEVED), jnp.float32),
            pltpu.VMEM((per * ENC_WIDTH, RETRIEVED), bf16),
            pltpu.SemaphoreType.DMA((per,)),
            pltpu.SemaphoreType.DMA((n_pieces[0],)),
        ],
        20,
        4 * per * RETRIEVED * ENC_WIDTH * widths[0],
        assign,
        owners,
        slots,
        store,
        *raw,
        *parts[0],
    )
    span_rows = NEIGHBOURS * RETRIEVED
    middle, across = call(
        functools.partial(cross_kernel, n_span, starts[1]),
        [shape(per * RETRIEVED, ENC_WIDTH)] * 2,
        [VMEM] * 7 + [HBM] * n_pieces[1],
        [VMEM] * 2,
        [
            pltpu.VMEM((ENC_WIDTH, widths[1]), bf16),
            pltpu.VMEM((rows_c, width_c), bf16),
            pltpu.VMEM((per * RETRIEVED, ENC_WIDTH), bf16),
            pltpu.VMEM((per * ENC_WIDTH, SPAN_LEN), jnp.float32),
            pltpu.VMEM((per * ENC_WIDTH, SPAN_LEN), bf16),
            pltpu.SemaphoreType.DMA((n_pieces[1],)),
        ],
        20,
        4 * per * RETRIEVED * ENC_WIDTH * widths[1],
        source,
        within,
        *context,
        *parts[1],
    )
    enc = call(
        functools.partial(encoded_kernel, n_span, starts[2]),
        [shape(span_rows, ENC_WIDTH)] * own_spans,
        [VMEM] * 2 + [HBM] * n_pieces[2],
        [VMEM] * own_spans,
        [
            pltpu.VMEM((ENC_WIDTH, widths[2]), bf16),
            pltpu.SemaphoreType.DMA((n_pieces[2],)),
        ],
        16,
        4 * per * RETRIEVED * ENC_WIDTH * widths[2],
        middle,
        across,
        *parts[2],
    )
    first = own_spans // 2
    x = [to(1, e) for e in enc]
    y = [to(2, e) for e in enc]
    d = [to(2, x[i]) for i in range(first)]
    d += [to(1, y[i]) for i in range(first, own_spans)]

    queries = call(
        query_kernel,
        shape(tokens, local),
        [VMEM] * 5 + [HBM],
        VMEM,
        [
            pltpu.VMEM((4, feat, local), bf16),
            pltpu.VMEM((tokens, local), jnp.float32),
            pltpu.SemaphoreType.DMA((4,)),
        ],
        24,
        8 * tokens * feat * local,
        states,
        states_x,
        states_y,
        d0,
        d1,
        query_weight,
    )
    w_pair = neighbour_weight.reshape(ENC_WIDTH, 2 * local)
    encoded = (enc, x, y, d)

    def scratch(spans, rows):
        return [
            pltpu.VMEM((rows * SPAN_LEN, local), bf16),
            pltpu.VMEM((spans * span_rows, ENC_WIDTH), bf16),
            pltpu.VMEM((spans * span_rows, 2 * local), bf16),
            pltpu.VMEM((spans * SPAN_LEN * local // HEAD_DIM, span_rows), jnp.float32),
            pltpu.VMEM((spans * SPAN_LEN * local // HEAD_DIM, span_rows), bf16),
            pltpu.SemaphoreType.DMA((spans,)),
        ]

    terms = []
    for chunk, early in zip(CHUNKS, ((), (0, 2))):
        rows = len(chunk) * SPAN_LEN
        given = []
        if early:
            spans = [chunk[s] for s in early]
            given.append(
                call(
                    functools.partial(early_kernel, spans),
                    shape(len(early) * SPAN_LEN, local),
                    [SMEM, HBM] + [VMEM] * (len(early) + 1),
                    VMEM,
                    scratch(len(early), len(early)),
                    24,
                    4 * len(early) * span_rows * ENC_WIDTH * 2 * local,
                    assign,
                    queries,
                    *(encoded[relation][i] for relation, i in spans),
                    w_pair,
                )
            )
        late = [chunk[s] for s in range(len(chunk)) if s not in early]
        keep_a, keep_b, to_x, to_y = call(
            functools.partial(span_kernel, chunk, early),
            [shape(rows // 2, 2 * feat)] * 4,
            [SMEM, HBM] + [VMEM] * (len(late) + len(given) + 2),
            [VMEM] * 4,
            [pltpu.VMEM((rows, local), bf16)] + scratch(len(late), len(chunk)),
            32,
            4 * len(late) * span_rows * ENC_WIDTH * 2 * local,
            assign,
            queries,
            *(encoded[relation][i] for relation, i in late),
            *given,
            w_pair,
            output_weight,
        )
        near_x, near_y = to(1, to_x), to(2, to_y)
        last_y = to(2, add(keep_a[:, feat:], near_x[:, feat:]))
        last_x = to(1, add(keep_b[:, feat:], near_y[:, feat:]))
        terms += [keep_a, keep_b, near_x, near_y, last_y, last_x]
    return call(
        final_kernel,
        shape(tokens, feat),
        [SMEM] + [VMEM] * 13,
        VMEM,
        [],
        16,
        17 * tokens * feat,
        assign,
        states,
        *terms,
    )


def solution(mesh):
    sizes = mesh.shape
    n_head, n_span = sizes["head"], sizes["span"]
    square = n_head == 4 and sizes["group"] == 2 and n_span >= 3

    def per_device(*args):
        spans = args[1].shape[0]
        if square and spans == 2 * n_head:
            return fast(n_span, *args)
        return general(*args)

    in_specs = (
        P(("span", "group"), "head"),
        P(("span", "group"), None),
        P(("span", "group"), None),
        P("span", "head", "group", None, None, None),
        P(("span", "group"), None),
        P("head", None),
        P(None, "head"),
        P(None, None, "head"),
        P("head", None),
    )
    out_specs = P(("span", "group"), "head")
    return jax.shard_map(
        per_device, mesh=mesh, in_specs=in_specs, out_specs=out_specs, check_vma=False
    )
```

```python
import functools

import jax
import jax.numpy as jnp
import numpy as np
from jax import lax
from jax.experimental import pallas as pl
from jax.experimental.pallas import tpu as pltpu
from jax.sharding import PartitionSpec as P


HEAD_DIM = 128
ENC_WIDTH = 896
SPAN_LEN = 64
RETRIEVED = 128
NEIGHBOURS = 2


HBM = pl.BlockSpec(memory_space=pltpu.HBM)
VMEM = pl.BlockSpec(memory_space=pltpu.VMEM)
SMEM = pl.BlockSpec(memory_space=pltpu.SMEM)


def attend(queries, keys_in, values_in, factor):
    scores = (
        jnp.einsum("bqhe,bkhe->bhqk", queries, keys_in, preferred_element_type=jnp.float32) * factor
    )
    weights = jax.nn.softmax(scores, axis=-1).astype(jnp.bfloat16)
    result = jnp.einsum("bhqk,bkhe->bqhe", weights, values_in, preferred_element_type=jnp.float32)
    return result.astype(jnp.bfloat16)


def encode(source, context, weights):
    number, length, breadth = source.shape
    groups = breadth // HEAD_DIM
    factor = HEAD_DIM ** (-0.5)
    rows_in = source.reshape(number * length, breadth)
    triple = jnp.dot(rows_in, weights[:, : 3 * breadth], preferred_element_type=jnp.float32).astype(
        jnp.bfloat16
    )
    triple = triple.reshape(number, length, 3, groups, HEAD_DIM)
    within = attend(triple[:, :, 0], triple[:, :, 1], triple[:, :, 2], factor).reshape(
        number * length, breadth
    )
    middle = rows_in.astype(jnp.float32) + jnp.dot(
        within, weights[:, 3 * breadth : 4 * breadth], preferred_element_type=jnp.float32
    )
    middle = middle.astype(jnp.bfloat16)
    asking = jnp.dot(
        middle, weights[:, 4 * breadth : 5 * breadth], preferred_element_type=jnp.float32
    ).astype(jnp.bfloat16)
    asking = asking.reshape(number, length, groups, HEAD_DIM)
    paired = context.reshape(number, context.shape[1], 2, groups, HEAD_DIM)
    across = attend(asking, paired[:, :, 0], paired[:, :, 1], factor).reshape(
        number * length, breadth
    )
    result = middle.astype(jnp.float32) + jnp.dot(
        across, weights[:, 5 * breadth :], preferred_element_type=jnp.float32
    )
    return result.astype(jnp.bfloat16).reshape(number, length, breadth)


def general(
    states,
    owners,
    places,
    stored,
    encoder_weights,
    context_weight,
    query_weight,
    neighbour_weight,
    output_weight,
):
    position = lax.axis_index("head")
    token_rows = states.shape[0]
    span_count = owners.shape[0]
    pair_count = span_count * NEIGHBOURS
    local_width = query_weight.shape[1]
    local_heads = local_width // HEAD_DIM
    factor = HEAD_DIM ** (-0.5)
    query_sums = jnp.dot(
        lax.all_gather(states, "head", axis=1, tiled=True),
        query_weight,
        preferred_element_type=jnp.float32,
    )
    queries = query_sums.astype(jnp.bfloat16)
    partial_context = jnp.dot(states, context_weight, preferred_element_type=jnp.float32)
    context = lax.psum(partial_context.astype(jnp.bfloat16), "head")
    context = context.reshape(span_count, SPAN_LEN, 2 * ENC_WIDTH)
    weights_all = lax.all_gather(encoder_weights, ("span", "group"), axis=0, tiled=True)
    owner_flat = owners.reshape(pair_count)
    place_flat = places.reshape(pair_count)
    pair_ids = jnp.arange(pair_count, dtype=jnp.int32)
    local_store = stored.reshape(stored.shape[3], stored.shape[4], stored.shape[5])
    slot_count = local_store.shape[0]
    slot_ids = jnp.arange(slot_count, dtype=jnp.int32)
    matched = (owner_flat[None, :] == position) & (place_flat[None, :] == slot_ids[:, None])
    span_of = jnp.sum(jnp.where(matched, pair_ids[None, :] // NEIGHBOURS, 0), axis=1)
    encoded = encode(local_store, context[span_of], weights_all)
    local_pair = neighbour_weight.reshape(ENC_WIDTH, 2 * local_width)
    piece = lax.all_gather(encoded, "head", axis=0, tiled=True)
    rows_in = piece.reshape(piece.shape[0] * RETRIEVED, ENC_WIDTH)
    result = jnp.dot(rows_in, local_pair, preferred_element_type=jnp.float32).astype(jnp.bfloat16)
    gathered = result.reshape(piece.shape[0], RETRIEVED, 2 * local_width)
    neighbour_pairs = gathered[owner_flat * slot_count + place_flat]
    asked = queries.reshape(span_count, SPAN_LEN, local_heads, HEAD_DIM)
    memory = neighbour_pairs.reshape(span_count, NEIGHBOURS * RETRIEVED, 2, local_heads, HEAD_DIM)
    attended = attend(asked, memory[:, :, 0], memory[:, :, 1], factor).reshape(
        token_rows, local_width
    )
    terms = jnp.dot(attended, output_weight, preferred_element_type=jnp.float32)
    summed = lax.psum_scatter(
        terms.astype(jnp.bfloat16), "head", scatter_dimension=1, tiled=True
    ).astype(jnp.float32)
    return (states.astype(jnp.float32) + summed).astype(jnp.bfloat16)


def call(kernel, out_shape, in_specs, out_specs, scratch, mib, flops, *args, aliases=()):
    return pl.pallas_call(
        kernel,
        out_shape=out_shape,
        in_specs=in_specs,
        out_specs=out_specs,
        scratch_shapes=scratch,
        input_output_aliases=dict(aliases),
        compiler_params=pltpu.CompilerParams(vmem_limit_bytes=mib * 1024 * 1024),
        cost_estimate=pl.CostEstimate(
            flops=flops,
            bytes_accessed=2 * sum(a.size for a in args),
            transcendentals=0,
        ),
    )(*args)


def dot(a, b):
    return jnp.dot(a, b, preferred_element_type=jnp.float32)


def attend_many(units, scores, weights):
    rows = scores.shape[0] // len(units)
    part = [slice(i * rows, (i + 1) * rows) for i in range(len(units))]
    factor = HEAD_DIM ** (-0.5)
    for at, (q, k, _, _) in zip(part, units):
        scores[at, :] = lax.dot_general(
            q(), k(), (((1,), (1,)), ((), ())), preferred_element_type=jnp.float32
        )
    for at in part:
        one = scores[at, :]
        top = jnp.max(one, axis=-1, keepdims=True)
        weights[at, :] = jnp.exp((one - top) * factor).astype(jnp.bfloat16)
    for at, (_, _, v, put) in zip(part, units):
        values = v()
        both = dot(weights[at, :], jnp.concatenate([values, jnp.ones_like(values)], axis=1))
        put((both[:, :HEAD_DIM] / both[:, HEAD_DIM:]).astype(jnp.bfloat16))


def unit(q, q_rows, q_col, k, k_rows, k_col, v_col, out):
    def put(value):
        out[q_rows, q_col : q_col + HEAD_DIM] = value

    return (
        lambda: q[q_rows, q_col : q_col + HEAD_DIM],
        lambda: k[k_rows, k_col : k_col + HEAD_DIM],
        lambda: k[k_rows, v_col : v_col + HEAD_DIM],
        put,
    )


def head_index():
    return lax.axis_index("head").astype(jnp.int32)


def square_place():
    me = head_index()
    return me % 2, me // 2


def cut_kernel(weights, query_part, half_part, last_part, sems):
    _, y = square_place()
    width = half_part.shape[1]
    first = query_part.shape[1]
    copies = []
    for i, (start, part) in enumerate(
        ((0, query_part), (first + y * width, half_part), (first + 2 * width, last_part))
    ):
        cols = pl.ds(pl.multiple_of(start, HEAD_DIM), part.shape[1])
        copies.append(pltpu.make_async_copy(weights.at[:, cols], part, sems.at[i]))
    for c in copies:
        c.start()
    for c in copies:
        c.wait()


def halves_kernel(states, *rest):
    outs, sems = rest[:-1], rest[-1]
    rows = outs[0].shape[0]
    copies = []
    for i, out in enumerate(outs):
        part = states.at[pl.ds(i * rows, rows), :]
        copies.append(pltpu.make_async_copy(part, out, sems.at[i]))
        copies[-1].start()
    for c in copies:
        c.wait()


def pairings(items):
    if not items:
        yield ()
        return
    for other in items[1:]:
        rest = tuple(i for i in items[1:] if i != other)
        for more in pairings(rest):
            yield ((items[0], other),) + more


def pair_table(spans):
    every = list(pairings(tuple(range(spans))))
    table = np.full((spans, -(-len(every) // 128) * 128), -1, np.int32)
    for c, pairing in enumerate(every):
        for slot, pair in enumerate(pairing):
            for span in pair:
                table[span, c] = slot
    return table


def plan_kernel(owners, table, assign):
    spans = table.shape[0]
    devices = spans // 2
    shape_row = (1, table.shape[1])
    hits = [
        [sum((owners[n, s] == o).astype(jnp.int32) for n in range(NEIGHBOURS)) for s in range(spans)]
        for o in range(devices)
    ]
    rows = [table[s : s + 1, :] for s in range(spans)]
    inside = [[(r == slot).astype(jnp.int32) for r in rows] for slot in range(devices)]
    fits = rows[0] >= 0
    for o in range(devices):
        heavy = jnp.zeros(shape_row, jnp.int32)
        for slot in range(devices):
            count = jnp.zeros(shape_row, jnp.int32)
            for s in range(spans):
                count = count + inside[slot][s] * hits[o][s]
            heavy = heavy + (count >= 3).astype(jnp.int32)
        fits = fits & (heavy <= 1)
    code = jnp.zeros(shape_row, jnp.int32)
    for s in range(spans):
        code = code + rows[s] * (devices**s)
    worst = devices**spans
    chosen = jnp.min(jnp.where(fits, code, worst).astype(jnp.float32)).astype(jnp.int32)
    slot_of = []
    for s in range(spans):
        slot_of.append(lax.rem(chosen, devices))
        chosen = lax.div(chosen, devices)
    takes = []
    for slot in range(devices):
        taker = jnp.int32(-1)
        for o in range(devices):
            count = sum(jnp.where(slot_of[s] == slot, hits[o][s], 0) for s in range(spans))
            taker = jnp.where(count >= 3, o, taker)
        takes.append(taker)
    for slot in range(devices):
        free = jnp.int32(0)
        for d in reversed(range(devices)):
            taken = sum((t == d).astype(jnp.int32) for t in takes)
            free = jnp.where(taken == 0, d, free)
        takes[slot] = jnp.where(takes[slot] < 0, free, takes[slot])
    for s in range(spans):
        before = sum(((slot_of[t] == slot_of[s]).astype(jnp.int32) for t in range(s)), jnp.int32(0))
        device = jnp.int32(0)
        for slot in range(devices):
            device = jnp.where(slot_of[s] == slot, takes[slot], device)
        assign[device * 2 + before] = jnp.int32(s)


def neighbours_of(assign, owners, places, device):
    found = []
    for j in range(2 * NEIGHBOURS):
        span = assign[device * 2 + j // NEIGHBOURS]
        found.append((owners[j % NEIGHBOURS, span], places[j % NEIGHBOURS, span]))
    return found


def pick_kernel(assign, owners, places, store, *rest):
    outs, (buf, sem_in, sem_out) = rest[:3], rest[3:]
    me = head_index()
    most = outs[0].shape[0]
    ins, puts = [], []
    for i in range(3):
        slots = [jnp.int32(0)] * most
        count = jnp.int32(0)
        for owner, place in neighbours_of(assign, owners, places, me ^ (i + 1)):
            here = owner == me
            for c in range(most):
                slots[c] = jnp.where(here & (count == c), place, slots[c])
            count = count + here.astype(jnp.int32)
        for c in range(most):
            k = i * most + c
            ins.append(pltpu.make_async_copy(store.at[slots[c]], buf.at[k], sem_in.at[k]))
            puts.append(pltpu.make_async_copy(buf.at[k], outs[i].at[c], sem_out.at[k]))
            ins[-1].start()
    for get, put in zip(ins, puts):
        get.wait()
        put.start()
    for c in puts:
        c.wait()


def context_kernel(assign, x, w, own, to_x, to_y, for_y, for_x, buf, sems):
    me = head_index()
    width = w.shape[1]
    half = width // 2
    for c in range(2):
        cols = slice(c * half, (c + 1) * half)
        buf[:, cols] = dot(x[...], w[:, cols]).astype(jnp.bfloat16)
    copies = []
    for out, parts in (
        (to_x, ((1, 0), (3, 0))),
        (to_y, ((2, 1), (3, 1))),
        (for_y, ((2, 0),)),
        (for_x, ((1, 1),)),
        (own, ((0, 0), (0, 1))),
    ):
        for n, (k, i) in enumerate(parts):
            start = pl.multiple_of(assign[(me ^ k) * 2 + i] * SPAN_LEN, SPAN_LEN)
            rows = out.at[pl.ds(n * SPAN_LEN, SPAN_LEN), :]
            part = buf.at[pl.ds(start, SPAN_LEN), :]
            copies.append(pltpu.make_async_copy(part, rows, sems.at[len(copies)]))
            copies[-1].start()
    for c in copies:
        c.wait()


def load_pieces(n_span, first, pieces, held, sems, begin=0, total=None):
    z = lax.axis_index("span").astype(jnp.int32)
    g = lax.axis_index("group").astype(jnp.int32)
    x, y = square_place()
    rows = pieces[0].shape[0]
    copies = []
    total = total or len(pieces)
    split = (total - 2) // (2 * (n_span - 1))
    for i, piece in enumerate(pieces, begin):
        if i < 2:
            r, other, cols = 0, i, slice(None)
            piece = piece.at[:, pl.ds(first, held.shape[1])]
        else:
            r, rest = 1 + (i - 2) // (2 * split), (i - 2) % (2 * split)
            other = rest % 2
            cols = slice(None)
            if split == 2:
                place = y if half_axis(n_span, r) else x
                block = place if rest < 2 else 1 - place
                width = held.shape[1] // 2
                cols = pl.ds(pl.multiple_of(block * width, width), width)
        spot = lax.rem(z + (n_span - r), n_span) * 2 + (g ^ other)
        start = pl.multiple_of(spot * rows, rows)
        copies.append(
            pltpu.make_async_copy(piece, held.at[pl.ds(start, rows), cols], sems.at[i - begin])
        )
    return copies


def half_axis(n_span, r):
    return min(r, n_span - 2) % 2


def early_weights_kernel(n_span, first, total, *rest):
    pieces, (held, sem_w) = rest[:-2], rest[-2:]
    copies = load_pieces(n_span, first, pieces, held, sem_w, total=total)
    for c in copies:
        c.start()
    for c in copies:
        c.wait()


def source_kernel(assign, owners, places, store, r1, r2, r3, source, sem_s):
    me = head_index()
    mine = neighbours_of(assign, owners, places, me)
    for j, (owner, place) in enumerate(mine):
        at = source.at[pl.ds(j * RETRIEVED, RETRIEVED), :]
        relation = owner ^ me
        nth = sum(((mine[t][0] == owner).astype(jnp.int32) for t in range(j)), jnp.int32(0))
        nth = jnp.minimum(nth, r1.shape[0] - 1)
        for k, ref in enumerate((store, r1, r2, r3)):

            @pl.when(relation == k)
            def _():
                pltpu.make_async_copy(ref.at[place if k == 0 else nth], at, sem_s.at[j]).start()

    for j in range(len(mine)):
        at = source.at[pl.ds(j * RETRIEVED, RETRIEVED), :]
        pltpu.make_async_copy(r1.at[0], at, sem_s.at[j]).wait()


def self_kernel(n_span, source, early, own, other, within, held, triple, scores, weights, sem_w):
    total = 2 * n_span
    copies = load_pieces(n_span, 0, (own, other), held, sem_w, begin=total - 2, total=total)
    for c in copies:
        c.start()
    for c in copies:
        c.wait()
    breadth = source.shape[1]
    for c in range(3):
        cols = slice(c * breadth, (c + 1) * breadth)
        triple[:, cols] = dot(source[...], held[:, cols]).astype(jnp.bfloat16)
    units = []
    for j in range(source.shape[0] // RETRIEVED):
        rows = slice(j * RETRIEVED, (j + 1) * RETRIEVED)
        for c in range(0, breadth, HEAD_DIM):
            units.append(unit(triple, rows, c, triple, rows, breadth + c, 2 * breadth + c, within))
    attend_many(units, scores, weights)


def cross_kernel(n_span, total, source, within, own, from_x, from_y, last_y, last_x, *rest):
    pieces = rest[1:5]
    middle, across, held, context, asking, scores, weights, sem_w = rest[5:]
    copies = load_pieces(n_span, 0, pieces, held, sem_w, begin=total - 4, total=total)
    for c in copies:
        c.start()
    breadth = source.shape[1]
    for i, (near, far) in enumerate(((from_x, last_y), (from_y, last_x))):
        at = slice(i * SPAN_LEN, (i + 1) * SPAN_LEN)
        sums = own[at, :].astype(jnp.float32) + near[:SPAN_LEN, :].astype(jnp.float32)
        context[at, :] = (sums + far[...].astype(jnp.float32)).astype(jnp.bfloat16)
    for c in copies:
        c.wait()
    middle[...] = (
        source[...].astype(jnp.float32) + dot(within[...], held[:, :breadth])
    ).astype(jnp.bfloat16)
    asking[...] = dot(middle[...], held[:, breadth:]).astype(jnp.bfloat16)
    span_rows = NEIGHBOURS * RETRIEVED
    units = []
    for s in range(2):
        rows = slice(s * span_rows, (s + 1) * span_rows)
        keys = slice(s * SPAN_LEN, (s + 1) * SPAN_LEN)
        for c in range(0, breadth, HEAD_DIM):
            units.append(unit(asking, rows, c, context, keys, c, breadth + c, across))
    attend_many(units, scores, weights)


def encoded_kernel(n_span, middle, across, early, own, other, *rest):
    outs, held, sem_w = rest[:-2], rest[-2], rest[-1]
    total = 2 * n_span
    copies = load_pieces(n_span, 0, (own, other), held, sem_w, begin=total - 2, total=total)
    for c in copies:
        c.start()
    for c in copies:
        c.wait()
    span_rows = NEIGHBOURS * RETRIEVED
    for s, out in enumerate(outs):
        rows = slice(s * span_rows, (s + 1) * span_rows)
        result = middle[rows, :].astype(jnp.float32) + dot(across[rows, :], held[...])
        out[...] = result.astype(jnp.bfloat16)


def query_kernel(own, x0, x1, y0, y1, d0, d1, w, out, held, total, sems):
    me = head_index()
    width = own.shape[1]
    half = d0.shape[0]
    copies = []
    for k in range(4):
        start = pl.multiple_of((me ^ k) * width, width)
        copies.append(
            pltpu.make_async_copy(w.at[pl.ds(start, width), :], held.at[k], sems.at[k])
        )
    for c in copies:
        c.start()
    copies[0].wait()
    total[...] = dot(own[...], held[0])
    for k, (first, second) in enumerate(((x0, x1), (y0, y1), (d0, d1))):
        copies[k + 1].wait()
        total[:half, :] += dot(first[...], held[k + 1])
        total[half:, :] += dot(second[...], held[k + 1])
    out[...] = total[...].astype(jnp.bfloat16)


CHUNKS = (((0, 0), (1, 0), (0, 1), (2, 1)), ((2, 0), (3, 0), (1, 1), (3, 1)))


def attend_spans(spans, assign, queries, encs, pair, att, rows_of, scratch):
    q, keep, memory, scores, weights, sem = scratch
    me = head_index()
    local = q.shape[1]
    span_rows = NEIGHBOURS * RETRIEVED
    loads = []
    for s, (relation, i) in enumerate(spans):
        span = assign[(me ^ relation) * 2 + i]
        at = pl.ds(pl.multiple_of(span * SPAN_LEN, SPAN_LEN), SPAN_LEN)
        to_rows = pl.ds(rows_of[s] * SPAN_LEN, SPAN_LEN)
        loads.append(pltpu.make_async_copy(queries.at[at, :], q.at[to_rows, :], sem.at[s]))
    for c in loads:
        c.start()
    for s in range(len(spans)):
        keep[s * span_rows : (s + 1) * span_rows, :] = encs[s][...]
    for c in range(2):
        cols = slice(c * local, (c + 1) * local)
        memory[:, cols] = dot(keep[...], pair[:, cols]).astype(jnp.bfloat16)
    for c in loads:
        c.wait()
    units = []
    for s in range(len(spans)):
        r = slice(rows_of[s] * SPAN_LEN, (rows_of[s] + 1) * SPAN_LEN)
        m = slice(s * span_rows, (s + 1) * span_rows)
        for c in range(0, local, HEAD_DIM):
            units.append(unit(q, r, c, memory, m, c, local + c, att))
    attend_many(units, scores, weights)


def early_kernel(spans, assign, queries, *rest):
    n = len(spans)
    attend_spans(spans, assign, queries, rest[:n], rest[n], rest[n + 1], range(n), rest[n + 2 :])


def span_kernel(chunk, early, assign, queries, *rest):
    late = [s for s in range(len(chunk)) if s not in early]
    n = len(late)
    encs, rest = rest[:n], rest[n:]
    if early:
        before, rest = rest[0], rest[1:]
    pair, held, keep_a, keep_b, to_x, to_y, att = rest[:7]
    me = head_index()
    for i, s in enumerate(early):
        att[s * SPAN_LEN : (s + 1) * SPAN_LEN, :] = before[i * SPAN_LEN : (i + 1) * SPAN_LEN, :]
    attend_spans([chunk[s] for s in late], assign, queries, encs, pair, att, late, rest[7:])
    width = keep_a.shape[1] // 2
    one = SPAN_LEN
    low, high = slice(0, width), slice(width, 2 * width)
    places = (
        ((keep_a, low, False), (keep_b, low, False)),
        ((to_x, low, True), (keep_b, high, False)),
        ((keep_a, high, False), (to_y, low, True)),
        ((to_x, high, True), (to_y, high, True)),
    )
    for k in range(4):
        start = pl.multiple_of((me ^ k) * width, width)
        term = dot(att[...], held[:, pl.ds(start, width)]).astype(jnp.bfloat16)
        for side, (out, cols, swapped) in enumerate(places[k]):
            first = term[2 * side * one : (2 * side + 1) * one, :]
            second = term[(2 * side + 1) * one : (2 * side + 2) * one, :]
            out[:one, cols] = second if swapped else first
            out[one:, cols] = first if swapped else second


def put_rows(assign, chunk, block, out, sems):
    me = head_index()
    copies = []
    for s, (relation, i) in enumerate(chunk):
        start = pl.multiple_of(assign[(me ^ relation) * 2 + i] * SPAN_LEN, SPAN_LEN)
        rows = block.at[pl.ds(s * SPAN_LEN, SPAN_LEN), :]
        copies.append(pltpu.make_async_copy(rows, out.at[pl.ds(start, SPAN_LEN), :], sems.at[s]))
        copies[-1].start()
    return copies


def almost_kernel(assign, states, *rest):
    kept, near, last = rest[:4], rest[4:8], rest[8:10]
    out, partial, block, sems = rest[10:]
    me = head_index()
    width = out.shape[1]
    for c in (1, 0):
        for s, (relation, i) in enumerate(CHUNKS[c]):
            side, row = s // 2, (s % 2) * SPAN_LEN
            part = slice(row, row + SPAN_LEN)
            start = pl.multiple_of(assign[(me ^ relation) * 2 + i] * SPAN_LEN, SPAN_LEN)
            total = kept[2 * c + side][part, :width].astype(jnp.float32)
            total = total + near[2 * c + side][part, :width].astype(jnp.float32)
            total = total + states[pl.ds(start, SPAN_LEN), :].astype(jnp.float32)
            rows = slice(s * SPAN_LEN, (s + 1) * SPAN_LEN)
            if c == 0:
                partial[rows, :] = total
            else:
                total = total + last[side][part, :].astype(jnp.float32)
                block[rows, :] = total.astype(jnp.bfloat16)
        if c == 1:
            copies = put_rows(assign, CHUNKS[c], block, out, sems)
    for c in copies:
        c.wait()


def final_kernel(assign, partial, last_y, last_x, before, out, block, sems):
    half = last_y.shape[0]
    for side, last in enumerate((last_y, last_x)):
        rows = slice(side * half, (side + 1) * half)
        block[rows, :] = (partial[rows, :] + last[...].astype(jnp.float32)).astype(jnp.bfloat16)
    for c in put_rows(assign, CHUNKS[0], block, out, sems):
        c.wait()


def shape(*dims):
    return jax.ShapeDtypeStruct(dims, jnp.bfloat16)


def add(a, b):
    return (a.astype(jnp.float32) + b.astype(jnp.float32)).astype(jnp.bfloat16)


def to(k, value):
    return lax.ppermute(value, "head", [(i, i ^ k) for i in range(4)])


def fast(
    n_span,
    states,
    owners,
    places,
    stored,
    encoder_weights,
    context_weight,
    query_weight,
    neighbour_weight,
    output_weight,
):
    bf16 = jnp.bfloat16
    tokens, feat = states.shape
    span_count = owners.shape[0]
    per = span_count * NEIGHBOURS // 4
    own_spans = span_count // 4
    local = query_weight.shape[1]
    store = stored.reshape(stored.shape[3], RETRIEVED, ENC_WIDTH)
    owners, slots = owners.T, places.T

    starts = (0, 3 * ENC_WIDTH, 5 * ENC_WIDTH)
    widths = (3 * ENC_WIDTH, 2 * ENC_WIDTH, ENC_WIDTH)
    rows_w = encoder_weights.shape[0]
    cut = call(
        cut_kernel,
        [shape(rows_w, widths[0]), shape(rows_w, ENC_WIDTH), shape(rows_w, ENC_WIDTH)],
        [HBM],
        [VMEM] * 3,
        [pltpu.SemaphoreType.DMA((3,))],
        60,
        2 * 10**9,
        encoder_weights,
    )
    h = lax.axis_index("head")
    places = (h % 2, h // 2)

    def ring(value):
        return lax.ppermute(value, "span", [(i, (i + 1) % n_span) for i in range(n_span)])

    def swap(value):
        return lax.ppermute(value, "group", [(0, 1), (1, 0)])

    partner = swap(encoder_weights)
    parts = [[encoder_weights, partner] for _ in starts]
    whole, near, last = cut
    far = None
    for r in range(1, n_span):
        whole = ring(whole)
        if r < n_span - 1:
            if r > 1:
                same = places[half_axis(n_span, r)] == places[half_axis(n_span, r - 1)]
                near = jnp.where(same, near, far)
            near = ring(near)
            far = to(1 + half_axis(n_span, r), near)
        else:
            near, far = ring(near), ring(far)
        last = ring(last)
        parts[0] += [whole, swap(whole)]
        parts[1] += [near, swap(near), far, swap(far)]
        parts[2] += [last, swap(last)]
    n_pieces = [len(p) for p in parts]

    table = jnp.asarray(pair_table(span_count))
    assign = pl.pallas_call(
        plan_kernel,
        out_shape=jax.ShapeDtypeStruct((span_count,), jnp.int32),
        in_specs=[SMEM, VMEM],
        out_specs=SMEM,
        name="plan",
    )(owners, table)

    most = 2
    sends = call(
        pick_kernel,
        [shape(most, RETRIEVED, ENC_WIDTH)] * 3,
        [SMEM] * 3 + [HBM],
        [HBM] * 3,
        [
            pltpu.VMEM((3 * most, RETRIEVED, ENC_WIDTH), bf16),
            pltpu.SemaphoreType.DMA((3 * most,)),
            pltpu.SemaphoreType.DMA((3 * most,)),
        ],
        60,
        4 * 10**9,
        assign,
        owners,
        slots,
        store,
    )
    raw = [to(k + 1, sends[k]) for k in range(3)]

    width_c = context_weight.shape[1]
    rows_c = own_spans * SPAN_LEN
    own_c, to_x, to_y, for_y, for_x = call(
        context_kernel,
        [shape(rows_c, width_c)] * 3 + [shape(SPAN_LEN, width_c)] * 2,
        [SMEM, VMEM, VMEM],
        [HBM] * 5,
        [pltpu.VMEM((tokens, width_c), bf16), pltpu.SemaphoreType.DMA((8,))],
        54,
        2 * tokens * feat * width_c,
        assign,
        states,
        context_weight,
    )
    from_x, from_y = to(1, to_x), to(2, to_y)
    last_y = add(for_y, from_x[SPAN_LEN:])
    last_x = add(for_x, from_y[SPAN_LEN:])
    last_y, last_x = to(2, last_y), to(1, last_x)
    context = [own_c, from_x, from_y, last_y, last_x]

    half_t = tokens // 2
    s0, s1 = call(
        halves_kernel,
        [shape(half_t, feat)] * 2,
        [HBM],
        [VMEM] * 2,
        [pltpu.SemaphoreType.DMA((2,))],
        60,
        2 * 10**9,
        states,
    )
    x0, y1 = to(1, s0), to(2, s1)
    x1, y0 = to(1, s1), to(2, s0)
    d0, d1 = to(2, x0), to(1, y1)

    held = []
    for i, n_last in enumerate((2, 4, 2)):
        n_early = n_pieces[i] - n_last
        held.append(
            call(
                functools.partial(early_weights_kernel, n_span, starts[i], n_pieces[i]),
                pltpu.VMEM((ENC_WIDTH, widths[i]), bf16),
                [HBM] * n_early,
                VMEM,
                [pltpu.SemaphoreType.DMA((n_early,))],
                16,
                2 * 10**9,
                *parts[i][:n_early],
            )
        )
    source = call(
        source_kernel,
        pltpu.VMEM((per * RETRIEVED, ENC_WIDTH), bf16),
        [SMEM] * 3 + [HBM] * 4,
        VMEM,
        [pltpu.SemaphoreType.DMA((per,))],
        16,
        2 * 10**9,
        assign,
        owners,
        slots,
        store,
        *raw,
    )
    within, _ = call(
        functools.partial(self_kernel, n_span),
        [
            pltpu.VMEM((per * RETRIEVED, ENC_WIDTH), bf16),
            pltpu.VMEM((ENC_WIDTH, widths[0]), bf16),
        ],
        [VMEM] * 2 + [HBM] * 2,
        [VMEM] * 2,
        [
            pltpu.VMEM((per * RETRIEVED, widths[0]), bf16),
            pltpu.VMEM((per * ENC_WIDTH, RETRIEVED), jnp.float32),
            pltpu.VMEM((per * ENC_WIDTH, RETRIEVED), bf16),
            pltpu.SemaphoreType.DMA((2,)),
        ],
        20,
        4 * per * RETRIEVED * ENC_WIDTH * widths[0],
        source,
        held[0],
        *parts[0][-2:],
        aliases={1: 1}.items(),
    )
    span_rows = NEIGHBOURS * RETRIEVED
    rows_e = per * RETRIEVED
    middle, across, _ = call(
        functools.partial(cross_kernel, n_span, n_pieces[1]),
        [pltpu.VMEM((rows_e, ENC_WIDTH), bf16)] * 2 + [pltpu.VMEM((ENC_WIDTH, widths[1]), bf16)],
        [VMEM] * 8 + [HBM] * 4,
        [VMEM] * 3,
        [
            pltpu.VMEM((rows_c, width_c), bf16),
            pltpu.VMEM((rows_e, ENC_WIDTH), bf16),
            pltpu.VMEM((per * ENC_WIDTH, SPAN_LEN), jnp.float32),
            pltpu.VMEM((per * ENC_WIDTH, SPAN_LEN), bf16),
            pltpu.SemaphoreType.DMA((4,)),
        ],
        20,
        4 * rows_e * ENC_WIDTH * widths[1],
        source,
        within,
        *context,
        held[1],
        *parts[1][-4:],
        aliases={7: 2}.items(),
    )
    *enc, _ = call(
        functools.partial(encoded_kernel, n_span),
        [shape(span_rows, ENC_WIDTH)] * own_spans + [pltpu.VMEM((ENC_WIDTH, widths[2]), bf16)],
        [VMEM] * 3 + [HBM] * 2,
        [VMEM] * (own_spans + 1),
        [pltpu.SemaphoreType.DMA((2,))],
        16,
        4 * rows_e * ENC_WIDTH * widths[2],
        middle,
        across,
        held[2],
        *parts[2][-2:],
        aliases={2: own_spans}.items(),
    )
    first = own_spans // 2
    x = [to(1, e) for e in enc]
    y = [to(2, e) for e in enc]
    d = [to(2, x[i]) for i in range(first)]
    d += [to(1, y[i]) for i in range(first, own_spans)]

    queries = call(
        query_kernel,
        shape(tokens, local),
        [VMEM] * 7 + [HBM],
        VMEM,
        [
            pltpu.VMEM((4, feat, local), bf16),
            pltpu.VMEM((tokens, local), jnp.float32),
            pltpu.SemaphoreType.DMA((4,)),
        ],
        24,
        8 * tokens * feat * local,
        states,
        x0,
        x1,
        y0,
        y1,
        d0,
        d1,
        query_weight,
    )
    w_pair = neighbour_weight.reshape(ENC_WIDTH, 2 * local)
    encoded = (enc, x, y, d)

    def scratch(spans, rows):
        return [
            pltpu.VMEM((rows * SPAN_LEN, local), bf16),
            pltpu.VMEM((spans * span_rows, ENC_WIDTH), bf16),
            pltpu.VMEM((spans * span_rows, 2 * local), bf16),
            pltpu.VMEM((spans * SPAN_LEN * local // HEAD_DIM, span_rows), jnp.float32),
            pltpu.VMEM((spans * SPAN_LEN * local // HEAD_DIM, span_rows), bf16),
            pltpu.SemaphoreType.DMA((spans,)),
        ]

    terms = []
    for chunk, early in zip(CHUNKS, ((), (0, 2))):
        rows = len(chunk) * SPAN_LEN
        given = []
        if early:
            spans = [chunk[s] for s in early]
            given.append(
                call(
                    functools.partial(early_kernel, spans),
                    shape(len(early) * SPAN_LEN, local),
                    [SMEM, HBM] + [VMEM] * (len(early) + 1),
                    VMEM,
                    scratch(len(early), len(early)),
                    24,
                    4 * len(early) * span_rows * ENC_WIDTH * 2 * local,
                    assign,
                    queries,
                    *(encoded[relation][i] for relation, i in spans),
                    w_pair,
                )
            )
        late = [chunk[s] for s in range(len(chunk)) if s not in early]
        keep_a, keep_b, to_x, to_y = call(
            functools.partial(span_kernel, chunk, early),
            [shape(rows // 2, 2 * feat)] * 4,
            [SMEM, HBM] + [VMEM] * (len(late) + len(given) + 2),
            [VMEM] * 4,
            [pltpu.VMEM((rows, local), bf16)] + scratch(len(late), len(chunk)),
            32,
            4 * len(late) * span_rows * ENC_WIDTH * 2 * local,
            assign,
            queries,
            *(encoded[relation][i] for relation, i in late),
            *given,
            w_pair,
            output_weight,
        )
        near_x, near_y = to(1, to_x), to(2, to_y)
        last_y = to(2, add(keep_a[:, feat:], near_x[:, feat:]))
        last_x = to(1, add(keep_b[:, feat:], near_y[:, feat:]))
        terms.append(((keep_a, keep_b), (near_x, near_y), (last_y, last_x)))
    (keep_1, near_1, last_1), (keep_2, near_2, last_2) = terms
    half_rows = tokens // 2
    rows_scratch = [pltpu.VMEM((half_rows, feat), bf16), pltpu.SemaphoreType.DMA((4,))]
    before, partial = call(
        almost_kernel,
        [shape(tokens, feat), pltpu.VMEM((half_rows, feat), jnp.float32)],
        [SMEM] + [VMEM] * 11,
        [HBM, VMEM],
        rows_scratch,
        16,
        17 * tokens * feat,
        assign,
        states,
        *keep_1,
        *keep_2,
        *near_1,
        *near_2,
        *last_1,
    )
    return call(
        final_kernel,
        shape(tokens, feat),
        [SMEM] + [VMEM] * 3 + [HBM],
        HBM,
        rows_scratch,
        16,
        4 * tokens * feat,
        assign,
        partial,
        *last_2,
        before,
        aliases={4: 0}.items(),
    )


def solution(mesh):
    sizes = mesh.shape
    n_head, n_span = sizes["head"], sizes["span"]
    square = n_head == 4 and sizes["group"] == 2 and n_span >= 3

    def per_device(*args):
        spans = args[1].shape[0]
        if square and spans == 2 * n_head:
            return fast(n_span, *args)
        return general(*args)

    in_specs = (
        P(("span", "group"), "head"),
        P(("span", "group"), None),
        P(("span", "group"), None),
        P("span", "head", "group", None, None, None),
        P(("span", "group"), None),
        P("head", None),
        P(None, "head"),
        P(None, None, "head"),
        P("head", None),
    )
    out_specs = P(("span", "group"), "head")
    return jax.shard_map(
        per_device, mesh=mesh, in_specs=in_specs, out_specs=out_specs, check_vma=False
    )
```

```python
import functools

import jax
import jax.numpy as jnp
import numpy as np
from jax import lax
from jax.experimental import pallas as pl
from jax.experimental.pallas import tpu as pltpu
from jax.sharding import PartitionSpec as P


HEAD_DIM = 128
ENC_WIDTH = 896
SPAN_LEN = 64
RETRIEVED = 128
NEIGHBOURS = 2


HBM = pl.BlockSpec(memory_space=pltpu.HBM)
VMEM = pl.BlockSpec(memory_space=pltpu.VMEM)
SMEM = pl.BlockSpec(memory_space=pltpu.SMEM)


def attend(queries, keys_in, values_in, factor):
    scores = (
        jnp.einsum("bqhe,bkhe->bhqk", queries, keys_in, preferred_element_type=jnp.float32) * factor
    )
    weights = jax.nn.softmax(scores, axis=-1).astype(jnp.bfloat16)
    result = jnp.einsum("bhqk,bkhe->bqhe", weights, values_in, preferred_element_type=jnp.float32)
    return result.astype(jnp.bfloat16)


def encode(source, context, weights):
    number, length, breadth = source.shape
    groups = breadth // HEAD_DIM
    factor = HEAD_DIM ** (-0.5)
    rows_in = source.reshape(number * length, breadth)
    triple = jnp.dot(rows_in, weights[:, : 3 * breadth], preferred_element_type=jnp.float32).astype(
        jnp.bfloat16
    )
    triple = triple.reshape(number, length, 3, groups, HEAD_DIM)
    within = attend(triple[:, :, 0], triple[:, :, 1], triple[:, :, 2], factor).reshape(
        number * length, breadth
    )
    middle = rows_in.astype(jnp.float32) + jnp.dot(
        within, weights[:, 3 * breadth : 4 * breadth], preferred_element_type=jnp.float32
    )
    middle = middle.astype(jnp.bfloat16)
    asking = jnp.dot(
        middle, weights[:, 4 * breadth : 5 * breadth], preferred_element_type=jnp.float32
    ).astype(jnp.bfloat16)
    asking = asking.reshape(number, length, groups, HEAD_DIM)
    paired = context.reshape(number, context.shape[1], 2, groups, HEAD_DIM)
    across = attend(asking, paired[:, :, 0], paired[:, :, 1], factor).reshape(
        number * length, breadth
    )
    result = middle.astype(jnp.float32) + jnp.dot(
        across, weights[:, 5 * breadth :], preferred_element_type=jnp.float32
    )
    return result.astype(jnp.bfloat16).reshape(number, length, breadth)


def general(
    states,
    owners,
    places,
    stored,
    encoder_weights,
    context_weight,
    query_weight,
    neighbour_weight,
    output_weight,
):
    position = lax.axis_index("head")
    token_rows = states.shape[0]
    span_count = owners.shape[0]
    pair_count = span_count * NEIGHBOURS
    local_width = query_weight.shape[1]
    local_heads = local_width // HEAD_DIM
    factor = HEAD_DIM ** (-0.5)
    query_sums = jnp.dot(
        lax.all_gather(states, "head", axis=1, tiled=True),
        query_weight,
        preferred_element_type=jnp.float32,
    )
    queries = query_sums.astype(jnp.bfloat16)
    partial_context = jnp.dot(states, context_weight, preferred_element_type=jnp.float32)
    context = lax.psum(partial_context.astype(jnp.bfloat16), "head")
    context = context.reshape(span_count, SPAN_LEN, 2 * ENC_WIDTH)
    weights_all = lax.all_gather(encoder_weights, ("span", "group"), axis=0, tiled=True)
    owner_flat = owners.reshape(pair_count)
    place_flat = places.reshape(pair_count)
    pair_ids = jnp.arange(pair_count, dtype=jnp.int32)
    local_store = stored.reshape(stored.shape[3], stored.shape[4], stored.shape[5])
    slot_count = local_store.shape[0]
    slot_ids = jnp.arange(slot_count, dtype=jnp.int32)
    matched = (owner_flat[None, :] == position) & (place_flat[None, :] == slot_ids[:, None])
    span_of = jnp.sum(jnp.where(matched, pair_ids[None, :] // NEIGHBOURS, 0), axis=1)
    encoded = encode(local_store, context[span_of], weights_all)
    local_pair = neighbour_weight.reshape(ENC_WIDTH, 2 * local_width)
    piece = lax.all_gather(encoded, "head", axis=0, tiled=True)
    rows_in = piece.reshape(piece.shape[0] * RETRIEVED, ENC_WIDTH)
    result = jnp.dot(rows_in, local_pair, preferred_element_type=jnp.float32).astype(jnp.bfloat16)
    gathered = result.reshape(piece.shape[0], RETRIEVED, 2 * local_width)
    neighbour_pairs = gathered[owner_flat * slot_count + place_flat]
    asked = queries.reshape(span_count, SPAN_LEN, local_heads, HEAD_DIM)
    memory = neighbour_pairs.reshape(span_count, NEIGHBOURS * RETRIEVED, 2, local_heads, HEAD_DIM)
    attended = attend(asked, memory[:, :, 0], memory[:, :, 1], factor).reshape(
        token_rows, local_width
    )
    terms = jnp.dot(attended, output_weight, preferred_element_type=jnp.float32)
    summed = lax.psum_scatter(
        terms.astype(jnp.bfloat16), "head", scatter_dimension=1, tiled=True
    ).astype(jnp.float32)
    return (states.astype(jnp.float32) + summed).astype(jnp.bfloat16)


def call(kernel, out_shape, in_specs, out_specs, scratch, mib, flops, *args, aliases=()):
    return pl.pallas_call(
        kernel,
        out_shape=out_shape,
        in_specs=in_specs,
        out_specs=out_specs,
        scratch_shapes=scratch,
        input_output_aliases=dict(aliases),
        compiler_params=pltpu.CompilerParams(vmem_limit_bytes=mib * 1024 * 1024),
        cost_estimate=pl.CostEstimate(
            flops=flops,
            bytes_accessed=2 * sum(a.size for a in args),
            transcendentals=0,
        ),
    )(*args)


def dot(a, b):
    return jnp.dot(a, b, preferred_element_type=jnp.float32)


def attend_many(units, scores, weights):
    rows = scores.shape[0] // len(units)
    part = [slice(i * rows, (i + 1) * rows) for i in range(len(units))]
    factor = HEAD_DIM ** (-0.5)
    for at, (q, k, _, _) in zip(part, units):
        scores[at, :] = lax.dot_general(
            q(), k(), (((1,), (1,)), ((), ())), preferred_element_type=jnp.float32
        )
    for at in part:
        one = scores[at, :]
        top = jnp.max(one, axis=-1, keepdims=True)
        weights[at, :] = jnp.exp((one - top) * factor).astype(jnp.bfloat16)
    for at, (_, _, v, put) in zip(part, units):
        values = v()
        both = dot(weights[at, :], jnp.concatenate([values, jnp.ones_like(values)], axis=1))
        put((both[:, :HEAD_DIM] / both[:, HEAD_DIM:]).astype(jnp.bfloat16))


def unit(q, q_rows, q_col, k, k_rows, k_col, v_col, out):
    def put(value):
        out[q_rows, q_col : q_col + HEAD_DIM] = value

    return (
        lambda: q[q_rows, q_col : q_col + HEAD_DIM],
        lambda: k[k_rows, k_col : k_col + HEAD_DIM],
        lambda: k[k_rows, v_col : v_col + HEAD_DIM],
        put,
    )


def head_index():
    return lax.axis_index("head").astype(jnp.int32)


def square_place():
    me = head_index()
    return me % 2, me // 2


def cut_kernel(weights, query_part, half_part, last_part, sems):
    _, y = square_place()
    width = half_part.shape[1]
    first = query_part.shape[1]
    copies = []
    for i, (start, part) in enumerate(
        ((0, query_part), (first + y * width, half_part), (first + 2 * width, last_part))
    ):
        cols = pl.ds(pl.multiple_of(start, HEAD_DIM), part.shape[1])
        copies.append(pltpu.make_async_copy(weights.at[:, cols], part, sems.at[i]))
    for c in copies:
        c.start()
    for c in copies:
        c.wait()


def halves_kernel(states, *rest):
    outs, sems = rest[:-1], rest[-1]
    rows = outs[0].shape[0]
    copies = []
    for i, out in enumerate(outs):
        part = states.at[pl.ds(i * rows, rows), :]
        copies.append(pltpu.make_async_copy(part, out, sems.at[i]))
        copies[-1].start()
    for c in copies:
        c.wait()


def pairings(items):
    if not items:
        yield ()
        return
    for other in items[1:]:
        rest = tuple(i for i in items[1:] if i != other)
        for more in pairings(rest):
            yield ((items[0], other),) + more


def pair_table(spans):
    every = list(pairings(tuple(range(spans))))
    table = np.full((spans, -(-len(every) // 128) * 128), -1, np.int32)
    for c, pairing in enumerate(every):
        for slot, pair in enumerate(pairing):
            for span in pair:
                table[span, c] = slot
    return table


def plan_kernel(owners, table, assign):
    spans = table.shape[0]
    devices = spans // 2
    shape_row = (1, table.shape[1])
    hits = [
        [sum((owners[n, s] == o).astype(jnp.int32) for n in range(NEIGHBOURS)) for s in range(spans)]
        for o in range(devices)
    ]
    rows = [table[s : s + 1, :] for s in range(spans)]
    inside = [[(r == slot).astype(jnp.int32) for r in rows] for slot in range(devices)]
    fits = rows[0] >= 0
    for o in range(devices):
        heavy = jnp.zeros(shape_row, jnp.int32)
        for slot in range(devices):
            count = jnp.zeros(shape_row, jnp.int32)
            for s in range(spans):
                count = count + inside[slot][s] * hits[o][s]
            heavy = heavy + (count >= 3).astype(jnp.int32)
        fits = fits & (heavy <= 1)
    code = jnp.zeros(shape_row, jnp.int32)
    for s in range(spans):
        code = code + rows[s] * (devices**s)
    worst = devices**spans
    chosen = jnp.min(jnp.where(fits, code, worst).astype(jnp.float32)).astype(jnp.int32)
    slot_of = []
    for s in range(spans):
        slot_of.append(lax.rem(chosen, devices))
        chosen = lax.div(chosen, devices)
    takes = []
    for slot in range(devices):
        taker = jnp.int32(-1)
        for o in range(devices):
            count = sum(jnp.where(slot_of[s] == slot, hits[o][s], 0) for s in range(spans))
            taker = jnp.where(count >= 3, o, taker)
        takes.append(taker)
    for slot in range(devices):
        free = jnp.int32(0)
        for d in reversed(range(devices)):
            taken = sum((t == d).astype(jnp.int32) for t in takes)
            free = jnp.where(taken == 0, d, free)
        takes[slot] = jnp.where(takes[slot] < 0, free, takes[slot])
    for s in range(spans):
        before = sum(((slot_of[t] == slot_of[s]).astype(jnp.int32) for t in range(s)), jnp.int32(0))
        device = jnp.int32(0)
        for slot in range(devices):
            device = jnp.where(slot_of[s] == slot, takes[slot], device)
        assign[device * 2 + before] = jnp.int32(s)


def neighbours_of(assign, owners, places, device):
    found = []
    for j in range(2 * NEIGHBOURS):
        span = assign[device * 2 + j // NEIGHBOURS]
        found.append((owners[j % NEIGHBOURS, span], places[j % NEIGHBOURS, span]))
    return found


def pick_kernel(assign, owners, places, store, *rest):
    outs, (buf, sem_in, sem_out) = rest[:3], rest[3:]
    me = head_index()
    most = outs[0].shape[0]
    ins, puts = [], []
    for i in range(3):
        slots = [jnp.int32(0)] * most
        count = jnp.int32(0)
        for owner, place in neighbours_of(assign, owners, places, me ^ (i + 1)):
            here = owner == me
            for c in range(most):
                slots[c] = jnp.where(here & (count == c), place, slots[c])
            count = count + here.astype(jnp.int32)
        for c in range(most):
            k = i * most + c
            ins.append(pltpu.make_async_copy(store.at[slots[c]], buf.at[k], sem_in.at[k]))
            puts.append(pltpu.make_async_copy(buf.at[k], outs[i].at[c], sem_out.at[k]))
            ins[-1].start()
    for get, put in zip(ins, puts):
        get.wait()
        put.start()
    for c in puts:
        c.wait()


def context_kernel(assign, x, w, own, to_x, to_y, for_y, for_x, buf, sems):
    me = head_index()
    width = w.shape[1]
    half = width // 2
    for c in range(2):
        cols = slice(c * half, (c + 1) * half)
        buf[:, cols] = dot(x[...], w[:, cols]).astype(jnp.bfloat16)
    copies = []
    for out, parts in (
        (to_x, ((1, 0), (3, 0))),
        (to_y, ((2, 1), (3, 1))),
        (for_y, ((2, 0),)),
        (for_x, ((1, 1),)),
        (own, ((0, 0), (0, 1))),
    ):
        for n, (k, i) in enumerate(parts):
            start = pl.multiple_of(assign[(me ^ k) * 2 + i] * SPAN_LEN, SPAN_LEN)
            rows = out.at[pl.ds(n * SPAN_LEN, SPAN_LEN), :]
            part = buf.at[pl.ds(start, SPAN_LEN), :]
            copies.append(pltpu.make_async_copy(part, rows, sems.at[len(copies)]))
            copies[-1].start()
    for c in copies:
        c.wait()


def load_pieces(n_span, first, pieces, held, sems, begin=0, total=None):
    z = lax.axis_index("span").astype(jnp.int32)
    g = lax.axis_index("group").astype(jnp.int32)
    x, y = square_place()
    rows = pieces[0].shape[0]
    copies = []
    total = total or len(pieces)
    split = (total - 2) // (2 * (n_span - 1))
    for i, piece in enumerate(pieces, begin):
        if i < 2:
            r, other, cols = 0, i, slice(None)
            piece = piece.at[:, pl.ds(first, held.shape[1])]
        else:
            r, rest = 1 + (i - 2) // (2 * split), (i - 2) % (2 * split)
            other = rest % 2
            cols = slice(None)
            if split == 2:
                place = y if half_axis(n_span, r) else x
                block = place if rest < 2 else 1 - place
                width = held.shape[1] // 2
                cols = pl.ds(pl.multiple_of(block * width, width), width)
        spot = lax.rem(z + (n_span - r), n_span) * 2 + (g ^ other)
        start = pl.multiple_of(spot * rows, rows)
        copies.append(
            pltpu.make_async_copy(piece, held.at[pl.ds(start, rows), cols], sems.at[i - begin])
        )
    return copies


def half_axis(n_span, r):
    return min(r, n_span - 2) % 2


def early_weights_kernel(n_span, first, total, *rest):
    pieces, (held, sem_w) = rest[:-2], rest[-2:]
    copies = load_pieces(n_span, first, pieces, held, sem_w, total=total)
    for c in copies:
        c.start()
    for c in copies:
        c.wait()


def source_kernel(assign, owners, places, store, r1, r2, r3, source, sem_s):
    me = head_index()
    mine = neighbours_of(assign, owners, places, me)
    for j, (owner, place) in enumerate(mine):
        at = source.at[pl.ds(j * RETRIEVED, RETRIEVED), :]
        relation = owner ^ me
        nth = sum(((mine[t][0] == owner).astype(jnp.int32) for t in range(j)), jnp.int32(0))
        nth = jnp.minimum(nth, r1.shape[0] - 1)
        for k, ref in enumerate((store, r1, r2, r3)):

            @pl.when(relation == k)
            def _():
                pltpu.make_async_copy(ref.at[place if k == 0 else nth], at, sem_s.at[j]).start()

    for j in range(len(mine)):
        at = source.at[pl.ds(j * RETRIEVED, RETRIEVED), :]
        pltpu.make_async_copy(r1.at[0], at, sem_s.at[j]).wait()


def self_kernel(n_span, source, early, own, other, within, held, triple, scores, weights, sem_w):
    total = 2 * n_span
    copies = load_pieces(n_span, 0, (own, other), held, sem_w, begin=total - 2, total=total)
    for c in copies:
        c.start()
    for c in copies:
        c.wait()
    breadth = source.shape[1]
    for c in range(3):
        cols = slice(c * breadth, (c + 1) * breadth)
        triple[:, cols] = dot(source[...], held[:, cols]).astype(jnp.bfloat16)
    units = []
    for j in range(source.shape[0] // RETRIEVED):
        rows = slice(j * RETRIEVED, (j + 1) * RETRIEVED)
        for c in range(0, breadth, HEAD_DIM):
            units.append(unit(triple, rows, c, triple, rows, breadth + c, 2 * breadth + c, within))
    attend_many(units, scores, weights)


def sums_kernel(own, from_x, from_y, last_y, last_x, context):
    for i, (near, far) in enumerate(((from_x, last_y), (from_y, last_x))):
        at = slice(i * SPAN_LEN, (i + 1) * SPAN_LEN)
        sums = own[at, :].astype(jnp.float32) + near[:SPAN_LEN, :].astype(jnp.float32)
        context[at, :] = (sums + far[...].astype(jnp.float32)).astype(jnp.bfloat16)


def cross_kernel(n_span, total, source, within, context, *rest):
    pieces = rest[1:5]
    middle, across, held, asking, scores, weights, sem_w = rest[5:]
    copies = load_pieces(n_span, 0, pieces, held, sem_w, begin=total - 4, total=total)
    for c in copies:
        c.start()
    breadth = source.shape[1]
    for c in copies:
        c.wait()
    middle[...] = (
        source[...].astype(jnp.float32) + dot(within[...], held[:, :breadth])
    ).astype(jnp.bfloat16)
    asking[...] = dot(middle[...], held[:, breadth:]).astype(jnp.bfloat16)
    span_rows = NEIGHBOURS * RETRIEVED
    units = []
    for s in range(2):
        rows = slice(s * span_rows, (s + 1) * span_rows)
        keys = slice(s * SPAN_LEN, (s + 1) * SPAN_LEN)
        for c in range(0, breadth, HEAD_DIM):
            units.append(unit(asking, rows, c, context, keys, c, breadth + c, across))
    attend_many(units, scores, weights)


def encoded_kernel(n_span, middle, across, early, own, other, *rest):
    outs, held, sem_w = rest[:-2], rest[-2], rest[-1]
    total = 2 * n_span
    copies = load_pieces(n_span, 0, (own, other), held, sem_w, begin=total - 2, total=total)
    for c in copies:
        c.start()
    for c in copies:
        c.wait()
    span_rows = NEIGHBOURS * RETRIEVED
    for s, out in enumerate(outs):
        rows = slice(s * span_rows, (s + 1) * span_rows)
        result = middle[rows, :].astype(jnp.float32) + dot(across[rows, :], held[...])
        out[...] = result.astype(jnp.bfloat16)


def query_kernel(own, x0, x1, y0, y1, d0, d1, w, out, held, total, sems):
    me = head_index()
    width = own.shape[1]
    half = d0.shape[0]
    copies = []
    for k in range(4):
        start = pl.multiple_of((me ^ k) * width, width)
        copies.append(
            pltpu.make_async_copy(w.at[pl.ds(start, width), :], held.at[k], sems.at[k])
        )
    for c in copies:
        c.start()
    copies[0].wait()
    total[...] = dot(own[...], held[0])
    for k, (first, second) in enumerate(((x0, x1), (y0, y1), (d0, d1))):
        copies[k + 1].wait()
        total[:half, :] += dot(first[...], held[k + 1])
        total[half:, :] += dot(second[...], held[k + 1])
    out[...] = total[...].astype(jnp.bfloat16)


CHUNKS = (((0, 0), (1, 0), (0, 1), (2, 1)), ((2, 0), (3, 0), (1, 1), (3, 1)))


def attend_spans(spans, assign, queries, encs, pair, att, rows_of, scratch):
    q, keep, memory, scores, weights, sem = scratch
    me = head_index()
    local = q.shape[1]
    span_rows = NEIGHBOURS * RETRIEVED
    loads = []
    for s, (relation, i) in enumerate(spans):
        span = assign[(me ^ relation) * 2 + i]
        at = pl.ds(pl.multiple_of(span * SPAN_LEN, SPAN_LEN), SPAN_LEN)
        to_rows = pl.ds(rows_of[s] * SPAN_LEN, SPAN_LEN)
        loads.append(pltpu.make_async_copy(queries.at[at, :], q.at[to_rows, :], sem.at[s]))
    for c in loads:
        c.start()
    for s in range(len(spans)):
        keep[s * span_rows : (s + 1) * span_rows, :] = encs[s][...]
    for c in range(2):
        cols = slice(c * local, (c + 1) * local)
        memory[:, cols] = dot(keep[...], pair[:, cols]).astype(jnp.bfloat16)
    for c in loads:
        c.wait()
    units = []
    for s in range(len(spans)):
        r = slice(rows_of[s] * SPAN_LEN, (rows_of[s] + 1) * SPAN_LEN)
        m = slice(s * span_rows, (s + 1) * span_rows)
        for c in range(0, local, HEAD_DIM):
            units.append(unit(q, r, c, memory, m, c, local + c, att))
    attend_many(units, scores, weights)


def early_kernel(spans, assign, queries, *rest):
    n = len(spans)
    attend_spans(spans, assign, queries, rest[:n], rest[n], rest[n + 1], range(n), rest[n + 2 :])


def span_kernel(chunk, early, assign, queries, *rest):
    late = [s for s in range(len(chunk)) if s not in early]
    n = len(late)
    encs, rest = rest[:n], rest[n:]
    if early:
        before, rest = rest[0], rest[1:]
    pair, held, keep_a, keep_b, to_x, to_y, att = rest[:7]
    me = head_index()
    for i, s in enumerate(early):
        att[s * SPAN_LEN : (s + 1) * SPAN_LEN, :] = before[i * SPAN_LEN : (i + 1) * SPAN_LEN, :]
    attend_spans([chunk[s] for s in late], assign, queries, encs, pair, att, late, rest[7:])
    width = keep_a.shape[1] // 2
    one = SPAN_LEN
    low, high = slice(0, width), slice(width, 2 * width)
    places = (
        ((keep_a, low, False), (keep_b, low, False)),
        ((to_x, low, True), (keep_b, high, False)),
        ((keep_a, high, False), (to_y, low, True)),
        ((to_x, high, True), (to_y, high, True)),
    )
    for k in range(4):
        start = pl.multiple_of((me ^ k) * width, width)
        term = dot(att[...], held[:, pl.ds(start, width)]).astype(jnp.bfloat16)
        for side, (out, cols, swapped) in enumerate(places[k]):
            first = term[2 * side * one : (2 * side + 1) * one, :]
            second = term[(2 * side + 1) * one : (2 * side + 2) * one, :]
            out[:one, cols] = second if swapped else first
            out[one:, cols] = first if swapped else second


def put_rows(assign, chunk, block, out, sems):
    me = head_index()
    copies = []
    for s, (relation, i) in enumerate(chunk):
        start = pl.multiple_of(assign[(me ^ relation) * 2 + i] * SPAN_LEN, SPAN_LEN)
        rows = block.at[pl.ds(s * SPAN_LEN, SPAN_LEN), :]
        copies.append(pltpu.make_async_copy(rows, out.at[pl.ds(start, SPAN_LEN), :], sems.at[s]))
        copies[-1].start()
    return copies


def almost_kernel(assign, states, *rest):
    kept, near, last = rest[:4], rest[4:8], rest[8:10]
    out, partial, block, sems = rest[10:]
    me = head_index()
    width = out.shape[1]
    for c in (1, 0):
        for s, (relation, i) in enumerate(CHUNKS[c]):
            side, row = s // 2, (s % 2) * SPAN_LEN
            part = slice(row, row + SPAN_LEN)
            start = pl.multiple_of(assign[(me ^ relation) * 2 + i] * SPAN_LEN, SPAN_LEN)
            total = kept[2 * c + side][part, :width].astype(jnp.float32)
            total = total + near[2 * c + side][part, :width].astype(jnp.float32)
            total = total + states[pl.ds(start, SPAN_LEN), :].astype(jnp.float32)
            rows = slice(s * SPAN_LEN, (s + 1) * SPAN_LEN)
            if c == 0:
                partial[rows, :] = total
            else:
                total = total + last[side][part, :].astype(jnp.float32)
                block[rows, :] = total.astype(jnp.bfloat16)
        if c == 1:
            copies = put_rows(assign, CHUNKS[c], block, out, sems)
    for c in copies:
        c.wait()


def final_kernel(assign, partial, last_y, last_x, before, out, block, sems):
    half = last_y.shape[0]
    for side, last in enumerate((last_y, last_x)):
        rows = slice(side * half, (side + 1) * half)
        block[rows, :] = (partial[rows, :] + last[...].astype(jnp.float32)).astype(jnp.bfloat16)
    for c in put_rows(assign, CHUNKS[0], block, out, sems):
        c.wait()


def shape(*dims):
    return jax.ShapeDtypeStruct(dims, jnp.bfloat16)


def add(a, b):
    return (a.astype(jnp.float32) + b.astype(jnp.float32)).astype(jnp.bfloat16)


def to(k, value):
    return lax.ppermute(value, "head", [(i, i ^ k) for i in range(4)])


def fast(
    n_span,
    states,
    owners,
    places,
    stored,
    encoder_weights,
    context_weight,
    query_weight,
    neighbour_weight,
    output_weight,
):
    bf16 = jnp.bfloat16
    tokens, feat = states.shape
    span_count = owners.shape[0]
    per = span_count * NEIGHBOURS // 4
    own_spans = span_count // 4
    local = query_weight.shape[1]
    store = stored.reshape(stored.shape[3], RETRIEVED, ENC_WIDTH)
    owners, slots = owners.T, places.T

    starts = (0, 3 * ENC_WIDTH, 5 * ENC_WIDTH)
    widths = (3 * ENC_WIDTH, 2 * ENC_WIDTH, ENC_WIDTH)
    rows_w = encoder_weights.shape[0]
    cut = call(
        cut_kernel,
        [shape(rows_w, widths[0]), shape(rows_w, ENC_WIDTH), shape(rows_w, ENC_WIDTH)],
        [HBM],
        [VMEM] * 3,
        [pltpu.SemaphoreType.DMA((3,))],
        60,
        2 * 10**9,
        encoder_weights,
    )
    h = lax.axis_index("head")
    places = (h % 2, h // 2)

    def ring(value):
        return lax.ppermute(value, "span", [(i, (i + 1) % n_span) for i in range(n_span)])

    def swap(value):
        return lax.ppermute(value, "group", [(0, 1), (1, 0)])

    partner = swap(encoder_weights)
    parts = [[encoder_weights, partner] for _ in starts]
    whole, near, last = cut
    far = None
    for r in range(1, n_span):
        whole = ring(whole)
        if r < n_span - 1:
            if r > 1:
                same = places[half_axis(n_span, r)] == places[half_axis(n_span, r - 1)]
                near = jnp.where(same, near, far)
            near = ring(near)
            far = to(1 + half_axis(n_span, r), near)
        else:
            near, far = ring(near), ring(far)
        last = ring(last)
        parts[0] += [whole, swap(whole)]
        parts[1] += [near, swap(near), far, swap(far)]
        parts[2] += [last, swap(last)]
    n_pieces = [len(p) for p in parts]

    table = jnp.asarray(pair_table(span_count))
    assign = pl.pallas_call(
        plan_kernel,
        out_shape=jax.ShapeDtypeStruct((span_count,), jnp.int32),
        in_specs=[SMEM, VMEM],
        out_specs=SMEM,
        name="plan",
    )(owners, table)

    most = 2
    sends = call(
        pick_kernel,
        [shape(most, RETRIEVED, ENC_WIDTH)] * 3,
        [SMEM] * 3 + [HBM],
        [HBM] * 3,
        [
            pltpu.VMEM((3 * most, RETRIEVED, ENC_WIDTH), bf16),
            pltpu.SemaphoreType.DMA((3 * most,)),
            pltpu.SemaphoreType.DMA((3 * most,)),
        ],
        60,
        4 * 10**9,
        assign,
        owners,
        slots,
        store,
    )
    raw = [to(k + 1, sends[k]) for k in range(3)]

    width_c = context_weight.shape[1]
    rows_c = own_spans * SPAN_LEN
    own_c, to_x, to_y, for_y, for_x = call(
        context_kernel,
        [shape(rows_c, width_c)] * 3 + [shape(SPAN_LEN, width_c)] * 2,
        [SMEM, VMEM, VMEM],
        [HBM] * 5,
        [pltpu.VMEM((tokens, width_c), bf16), pltpu.SemaphoreType.DMA((8,))],
        54,
        2 * tokens * feat * width_c,
        assign,
        states,
        context_weight,
    )
    from_x, from_y = to(1, to_x), to(2, to_y)
    last_y = add(for_y, from_x[SPAN_LEN:])
    last_x = add(for_x, from_y[SPAN_LEN:])
    last_y, last_x = to(2, last_y), to(1, last_x)
    context = call(
        sums_kernel,
        pltpu.VMEM((rows_c, width_c), bf16),
        [VMEM] * 5,
        VMEM,
        [],
        16,
        10**9,
        own_c,
        from_x,
        from_y,
        last_y,
        last_x,
    )

    half_t = tokens // 2
    s0, s1 = call(
        halves_kernel,
        [shape(half_t, feat)] * 2,
        [HBM],
        [VMEM] * 2,
        [pltpu.SemaphoreType.DMA((2,))],
        60,
        2 * 10**9,
        states,
    )
    x0, y1 = to(1, s0), to(2, s1)
    x1, y0 = to(1, s1), to(2, s0)
    d0, d1 = to(2, x0), to(1, y1)

    held = []
    for i, n_last in enumerate((2, 4, 2)):
        n_early = n_pieces[i] - n_last
        held.append(
            call(
                functools.partial(early_weights_kernel, n_span, starts[i], n_pieces[i]),
                pltpu.VMEM((ENC_WIDTH, widths[i]), bf16),
                [HBM] * n_early,
                VMEM,
                [pltpu.SemaphoreType.DMA((n_early,))],
                16,
                2 * 10**9,
                *parts[i][:n_early],
            )
        )
    source = call(
        source_kernel,
        pltpu.VMEM((per * RETRIEVED, ENC_WIDTH), bf16),
        [SMEM] * 3 + [HBM] * 4,
        VMEM,
        [pltpu.SemaphoreType.DMA((per,))],
        16,
        2 * 10**9,
        assign,
        owners,
        slots,
        store,
        *raw,
    )
    within, _ = call(
        functools.partial(self_kernel, n_span),
        [
            pltpu.VMEM((per * RETRIEVED, ENC_WIDTH), bf16),
            pltpu.VMEM((ENC_WIDTH, widths[0]), bf16),
        ],
        [VMEM] * 2 + [HBM] * 2,
        [VMEM] * 2,
        [
            pltpu.VMEM((per * RETRIEVED, widths[0]), bf16),
            pltpu.VMEM((per * ENC_WIDTH, RETRIEVED), jnp.float32),
            pltpu.VMEM((per * ENC_WIDTH, RETRIEVED), bf16),
            pltpu.SemaphoreType.DMA((2,)),
        ],
        20,
        4 * per * RETRIEVED * ENC_WIDTH * widths[0],
        source,
        held[0],
        *parts[0][-2:],
        aliases={1: 1}.items(),
    )
    span_rows = NEIGHBOURS * RETRIEVED
    rows_e = per * RETRIEVED
    middle, across, _ = call(
        functools.partial(cross_kernel, n_span, n_pieces[1]),
        [pltpu.VMEM((rows_e, ENC_WIDTH), bf16)] * 2 + [pltpu.VMEM((ENC_WIDTH, widths[1]), bf16)],
        [VMEM] * 4 + [HBM] * 4,
        [VMEM] * 3,
        [
            pltpu.VMEM((rows_e, ENC_WIDTH), bf16),
            pltpu.VMEM((per * ENC_WIDTH, SPAN_LEN), jnp.float32),
            pltpu.VMEM((per * ENC_WIDTH, SPAN_LEN), bf16),
            pltpu.SemaphoreType.DMA((4,)),
        ],
        20,
        4 * rows_e * ENC_WIDTH * widths[1],
        source,
        within,
        context,
        held[1],
        *parts[1][-4:],
        aliases={3: 2}.items(),
    )
    *enc, _ = call(
        functools.partial(encoded_kernel, n_span),
        [shape(span_rows, ENC_WIDTH)] * own_spans + [pltpu.VMEM((ENC_WIDTH, widths[2]), bf16)],
        [VMEM] * 3 + [HBM] * 2,
        [VMEM] * (own_spans + 1),
        [pltpu.SemaphoreType.DMA((2,))],
        16,
        4 * rows_e * ENC_WIDTH * widths[2],
        middle,
        across,
        held[2],
        *parts[2][-2:],
        aliases={2: own_spans}.items(),
    )
    first = own_spans // 2
    x = [to(1, e) for e in enc]
    y = [to(2, e) for e in enc]
    d = [to(2, x[i]) for i in range(first)]
    d += [to(1, y[i]) for i in range(first, own_spans)]

    queries = call(
        query_kernel,
        shape(tokens, local),
        [VMEM] * 7 + [HBM],
        VMEM,
        [
            pltpu.VMEM((4, feat, local), bf16),
            pltpu.VMEM((tokens, local), jnp.float32),
            pltpu.SemaphoreType.DMA((4,)),
        ],
        24,
        8 * tokens * feat * local,
        states,
        x0,
        x1,
        y0,
        y1,
        d0,
        d1,
        query_weight,
    )
    w_pair = neighbour_weight.reshape(ENC_WIDTH, 2 * local)
    encoded = (enc, x, y, d)

    def scratch(spans, rows):
        return [
            pltpu.VMEM((rows * SPAN_LEN, local), bf16),
            pltpu.VMEM((spans * span_rows, ENC_WIDTH), bf16),
            pltpu.VMEM((spans * span_rows, 2 * local), bf16),
            pltpu.VMEM((spans * SPAN_LEN * local // HEAD_DIM, span_rows), jnp.float32),
            pltpu.VMEM((spans * SPAN_LEN * local // HEAD_DIM, span_rows), bf16),
            pltpu.SemaphoreType.DMA((spans,)),
        ]

    terms = []
    for chunk, early in zip(CHUNKS, ((), (0, 2))):
        rows = len(chunk) * SPAN_LEN
        given = []
        if early:
            spans = [chunk[s] for s in early]
            given.append(
                call(
                    functools.partial(early_kernel, spans),
                    shape(len(early) * SPAN_LEN, local),
                    [SMEM, HBM] + [VMEM] * (len(early) + 1),
                    VMEM,
                    scratch(len(early), len(early)),
                    24,
                    4 * len(early) * span_rows * ENC_WIDTH * 2 * local,
                    assign,
                    queries,
                    *(encoded[relation][i] for relation, i in spans),
                    w_pair,
                )
            )
        late = [chunk[s] for s in range(len(chunk)) if s not in early]
        keep_a, keep_b, to_x, to_y = call(
            functools.partial(span_kernel, chunk, early),
            [shape(rows // 2, 2 * feat)] * 4,
            [SMEM, HBM] + [VMEM] * (len(late) + len(given) + 2),
            [VMEM] * 4,
            [pltpu.VMEM((rows, local), bf16)] + scratch(len(late), len(chunk)),
            32,
            4 * len(late) * span_rows * ENC_WIDTH * 2 * local,
            assign,
            queries,
            *(encoded[relation][i] for relation, i in late),
            *given,
            w_pair,
            output_weight,
        )
        near_x, near_y = to(1, to_x), to(2, to_y)
        last_y = to(2, add(keep_a[:, feat:], near_x[:, feat:]))
        last_x = to(1, add(keep_b[:, feat:], near_y[:, feat:]))
        terms.append(((keep_a, keep_b), (near_x, near_y), (last_y, last_x)))
    (keep_1, near_1, last_1), (keep_2, near_2, last_2) = terms
    half_rows = tokens // 2
    rows_scratch = [pltpu.VMEM((half_rows, feat), bf16), pltpu.SemaphoreType.DMA((4,))]
    before, partial = call(
        almost_kernel,
        [shape(tokens, feat), pltpu.VMEM((half_rows, feat), jnp.float32)],
        [SMEM] + [VMEM] * 11,
        [HBM, VMEM],
        rows_scratch,
        16,
        17 * tokens * feat,
        assign,
        states,
        *keep_1,
        *keep_2,
        *near_1,
        *near_2,
        *last_1,
    )
    return call(
        final_kernel,
        shape(tokens, feat),
        [SMEM] + [VMEM] * 3 + [HBM],
        HBM,
        rows_scratch,
        16,
        4 * tokens * feat,
        assign,
        partial,
        *last_2,
        before,
        aliases={4: 0}.items(),
    )


def solution(mesh):
    sizes = mesh.shape
    n_head, n_span = sizes["head"], sizes["span"]
    square = n_head == 4 and sizes["group"] == 2 and n_span >= 3

    def per_device(*args):
        spans = args[1].shape[0]
        if square and spans == 2 * n_head:
            return fast(n_span, *args)
        return general(*args)

    in_specs = (
        P(("span", "group"), "head"),
        P(("span", "group"), None),
        P(("span", "group"), None),
        P("span", "head", "group", None, None, None),
        P(("span", "group"), None),
        P("head", None),
        P(None, "head"),
        P(None, None, "head"),
        P("head", None),
    )
    out_specs = P(("span", "group"), "head")
    return jax.shard_map(
        per_device, mesh=mesh, in_specs=in_specs, out_specs=out_specs, check_vma=False
    )
```
